128 devices in a mesh: dom: 32 (over y, z, core), mp: 4 (over x).
Axes of the slice: x: 4, y: 4, z: 4, core: 2. Of those that a mesh axis runs over, the one named last changes fastest.
Arguments:
- grid_feat: bfloat16 [131072, 256], P(('dom', 'mp')), may hold values from -6 to 6
- grid_target: int32 [131072], P(('dom', 'mp')), may hold values from 0 to 32767, as said below
- enc_w1: bfloat16 [256, 512], replicated, may hold values from -0.375 to 0.375
- enc_b1: float32 [512], replicated, may hold values from -3 to 3
- enc_w2: bfloat16 [512, 512], replicated, may hold values from -0.25 to 0.25
- enc_gain: float32 [512], replicated, may hold values from 0.25 to 1.75
- mesh_embed: bfloat16 [32768, 512], P('dom', 'mp'), may hold values from -6 to 6
- nbr_blocks: int32 [512, 16], P('dom'), may hold values from 0 to 511, as said below
- attn_bias: float32 [8, 16, 32768], P('mp', None, 'dom'), may hold values from -2 to 300
- ln_gain: float32 [2, 2, 512], replicated, may hold values from 0.25 to 1.75
- qkv_w: bfloat16 [2, 3, 512, 512], P(None, None, None, 'mp'), may hold values from -0.25 to 0.25
- out_w: bfloat16 [2, 512, 512], P(None, 'mp'), may hold values from -0.25 to 0.25
- up_w: bfloat16 [2, 512, 2048], P(None, None, 'mp'), may hold values from -0.25 to 0.25
- down_w: bfloat16 [2, 2048, 512], P(None, 'mp'), may hold values from -0.125 to 0.125
Outputs:
- mesh_out: bfloat16 [32768, 512], P('dom', 'mp')
The draws below stay inside these ranges and needn't reach their ends.
Inputs may be any that keep to these rules, and one draw needn't show every extreme that they name: `grid_target`: among the 1024 grid nodes of one device (devices in the order dom, then mp), at most 64 have targets among the mesh nodes e * 1024 to (e + 1) * 1024 - 1 of one dom index e, and in every draw some dom index receives exactly 64 from every device. `nbr_blocks`: row b lists 16 different blocks, b itself among them, all within the 24 blocks that start at (b // 16) * 16 - 4, counted around the cycle of 512 blocks.
All inputs are finite; a program needn't handle non-finite values.
Results may differ from the reference program's by a relative error of at most 0.014.
Values may be sent and summed in bfloat16 or wider, within the bound.
No kernel may reach another device: no remote copies, remote signals or barrier semaphores. Data moves between devices by JAX's collectives and lax.ppermute only.
A program may use at most 128 MiB of HBM per device.

```python
import jax
import jax.numpy as jnp
from jax import lax

D = 512
HEADS = 8
HEAD_DIM = 64
FF = 2048
F_IN = 256
LAYERS = 2
BLK = 64
NBLK = 16
HB = 4
GR_DEV = 1024
BLOCKS_DEV = 16
CAP = 64
M_DEV = 1024
MESH = 32768
BLOCKS = 512
GRID = 131072
N_DOM = 32


def draw_grid_target(key, part):
    dom_total = MESH // M_DEV
    slot_total = dom_total * CAP
    spread_top = max(1, (1 << 29) // slot_total)
    key_full, key_rows = jax.random.split(jax.random.fold_in(key, 11))
    full_dom = jax.random.randint(key_full, (), 0, dom_total)

    def one_device(device_key):
        key_a, key_b, key_c = jax.random.split(device_key, 3)
        slot_ids = jnp.arange(slot_total, dtype=jnp.int32)
        scores = jax.random.randint(key_a, (slot_total,), 0, spread_top) * slot_total + slot_ids
        scores = jnp.where(slot_ids // CAP == full_dom, (1 << 30) + slot_ids, scores)
        chosen = lax.top_k(scores, GR_DEV)[1]
        chosen = chosen[jax.random.permutation(key_b, GR_DEV)]
        target_node = jax.random.randint(key_c, (GR_DEV,), 0, M_DEV)
        return (chosen // CAP * M_DEV + target_node).astype(jnp.int32)
    device_keys = jax.random.split(key_rows, GRID // GR_DEV)
    return jax.vmap(one_device)(device_keys).reshape(GRID)


def draw_nbr_blocks(key, part):
    window_span = BLOCKS_DEV + 2 * HB
    slot_ids = jnp.arange(window_span, dtype=jnp.int32)

    def one_block(block_id, block_key):
        device_id = block_id // BLOCKS_DEV
        own_slot = block_id - device_id * BLOCKS_DEV + HB
        scores = jax.random.randint(block_key, (window_span,), 0, 1 << 16) * window_span + slot_ids
        scores = jnp.where(slot_ids == own_slot, 1 << 30, scores)
        chosen = lax.top_k(scores, NBLK)[1]
        return ((device_id * BLOCKS_DEV - HB + chosen) % BLOCKS).astype(jnp.int32)
    block_keys = jax.random.split(jax.random.fold_in(key, 7), BLOCKS)
    return jax.vmap(one_block)(jnp.arange(BLOCKS, dtype=jnp.int32), block_keys)


def draw_attn_bias(key, part):
    key_a = jax.random.fold_in(jax.random.fold_in(key, 5), 0)
    base_bias = jax.random.uniform(key_a, (HEADS, NBLK, MESH), jnp.float32, -2.0, 2.0)
    return base_bias


def steps_of(stream_key, extent, pieces, smallest, high):
    def one(position, shards_of):
        draws = jax.random.uniform(jax.random.fold_in(jax.random.fold_in(stream_key, 6), position), (shards_of,), jnp.float32, smallest / len(pieces), high / len(pieces))
        return jnp.repeat(jnp.exp(draws), extent[position] // shards_of).reshape((-1,) + (1,) * (len(extent) - position - 1))

    gain = one(*pieces[0])
    for cut in pieces[1:]:
        gain = gain * one(*cut)
    return gain


def normal_values(rng, extent, scale, most, cuts=(), kind=jnp.bfloat16):
    factor_of = steps_of(rng, extent, cuts, -0.22, 0.18) if cuts else 1.0
    drawn = jax.random.normal(rng, extent, jnp.float32) * scale * factor_of
    return jnp.minimum(jnp.maximum(drawn, -most), most).astype(kind)


def setup_inputs(seed: int = 0) -> dict:
    key_of = jax.random.split(jax.random.key(seed), 15)
    return {
        "grid_feat": normal_values(key_of[0], (GRID, F_IN), 1.0, 6.0, ((0, 128),)),
        "grid_target": draw_grid_target(jax.random.fold_in(key_of[14], 71), 0),
        "enc_w1": normal_values(key_of[2], (F_IN, D), F_IN ** -0.5, 0.375),
        "enc_b1": normal_values(key_of[3], (D,), 0.5, 3.0, (), jnp.float32),
        "enc_w2": normal_values(key_of[4], (D, D), D ** -0.5, 0.25),
        "enc_gain": jnp.clip(1.0 + 0.15 * jax.random.normal(key_of[5], (D,), jnp.float32), 0.25, 1.75),
        "mesh_embed": normal_values(key_of[6], (MESH, D), 1.0, 6.0, ((0, 32), (1, 4))),
        "nbr_blocks": draw_nbr_blocks(jax.random.fold_in(key_of[14], 71), 0),
        "attn_bias": draw_attn_bias(jax.random.fold_in(key_of[14], 71), 0),
        "ln_gain": jnp.clip(1.0 + 0.15 * jax.random.normal(key_of[9], (LAYERS, 2, D), jnp.float32), 0.25, 1.75),
        "qkv_w": normal_values(key_of[10], (LAYERS, 3, D, D), D ** -0.5, 0.25, ((3, 4),)),
        "out_w": normal_values(key_of[11], (LAYERS, D, D), D ** -0.5, 0.25, ((1, 4),)),
        "up_w": normal_values(key_of[12], (LAYERS, D, FF), D ** -0.5, 0.25, ((2, 4),)),
        "down_w": normal_values(key_of[13], (LAYERS, FF, D), FF ** -0.5, 0.125, ((1, 4),)),
    }


EPS = 1e-05

def normalize(values, gain_vector):
    values = values.astype(jnp.float32)
    row_mean = lax.optimization_barrier(jnp.mean(values, axis=-1, keepdims=True))
    centered = values - row_mean
    variance = lax.optimization_barrier(jnp.mean(centered * centered, axis=-1, keepdims=True))
    return centered * lax.rsqrt(variance + EPS) * gain_vector

def encode(features, enc_w1, enc_b1, enc_w2, enc_gain):
    first = jnp.dot(features, enc_w1, preferred_element_type=jnp.float32) + enc_b1
    first = jax.nn.silu(first).astype(jnp.bfloat16)
    second = jnp.dot(first, enc_w2, preferred_element_type=jnp.float32)
    return normalize(second, enc_gain).astype(jnp.bfloat16)

def attend(queries, key_rows, value_rows, nbr_blocks, attn_bias):
    query_blocks = queries.reshape(N_DOM, BLOCKS_DEV, BLK, HEADS, HEAD_DIM)
    key_blocks = key_rows.reshape(BLOCKS, BLK, HEADS, HEAD_DIM)
    value_blocks = value_rows.reshape(BLOCKS, BLK, HEADS, HEAD_DIM)
    block_lists = nbr_blocks.reshape(N_DOM, BLOCKS_DEV, NBLK)
    bias_rows = jnp.transpose(attn_bias.reshape(HEADS, NBLK, N_DOM, BLOCKS_DEV, BLK), (2, 3, 0, 4, 1))

    def one_group(block_item):
        group_query, group_lists, group_bias = block_item
        group_keys = key_blocks[group_lists].reshape(BLOCKS_DEV, NBLK * BLK, HEADS, HEAD_DIM).astype(jnp.float32)
        group_values = value_blocks[group_lists].reshape(BLOCKS_DEV, NBLK * BLK, HEADS, HEAD_DIM).astype(jnp.float32)
        scores = jnp.einsum('tqhe,tkhe->thqk', group_query.astype(jnp.float32), group_keys) * HEAD_DIM ** (-0.5)
        scores = scores.reshape(BLOCKS_DEV, HEADS, BLK, NBLK, BLK) + group_bias[..., None]
        row_max = lax.optimization_barrier(jnp.max(scores, axis=(3, 4), keepdims=True))
        exponent = jnp.exp(scores - row_max)
        weights = (exponent / lax.optimization_barrier(jnp.sum(exponent, axis=(3, 4), keepdims=True))).astype(jnp.bfloat16)
        weights = weights.reshape(BLOCKS_DEV, HEADS, BLK, NBLK * BLK).astype(jnp.float32)
        attended = jnp.einsum('thqk,tkhe->tqhe', weights, group_values)
        return attended.astype(jnp.bfloat16).reshape(BLOCKS_DEV * BLK, HEADS * HEAD_DIM)
    return lax.map(one_group, (query_blocks, block_lists, bias_rows)).reshape(MESH, D)

def reference(grid_feat, grid_target, enc_w1, enc_b1, enc_w2, enc_gain, mesh_embed, nbr_blocks, attn_bias, ln_gain, qkv_w, out_w, up_w, down_w):
    features = grid_feat.reshape(GRID // GR_DEV, GR_DEV, F_IN)
    targets = grid_target.reshape(GRID // GR_DEV, GR_DEV)

    def add_block(running, block_item):
        message = encode(block_item[0], enc_w1, enc_b1, enc_w2, enc_gain)
        return (running.at[block_item[1]].add(message.astype(jnp.float32)), None)
    gathered, _ = lax.scan(add_block, jnp.zeros((MESH, D), jnp.float32), (features, targets))
    stream = (mesh_embed.astype(jnp.float32) + gathered).astype(jnp.bfloat16)
    for layer_index in range(LAYERS):
        normed = normalize(stream, ln_gain[layer_index, 0]).astype(jnp.bfloat16)
        queries = jnp.dot(normed, qkv_w[layer_index, 0], preferred_element_type=jnp.float32).astype(jnp.bfloat16)
        key_rows = jnp.dot(normed, qkv_w[layer_index, 1], preferred_element_type=jnp.float32).astype(jnp.bfloat16)
        value_rows = jnp.dot(normed, qkv_w[layer_index, 2], preferred_element_type=jnp.float32).astype(jnp.bfloat16)
        attended = attend(queries, key_rows, value_rows, nbr_blocks, attn_bias)
        stream = (stream.astype(jnp.float32) + jnp.dot(attended, out_w[layer_index], preferred_element_type=jnp.float32)).astype(jnp.bfloat16)
        normed = normalize(stream, ln_gain[layer_index, 1]).astype(jnp.bfloat16)
        hidden = jax.nn.silu(jnp.dot(normed, up_w[layer_index], preferred_element_type=jnp.float32)).astype(jnp.bfloat16)
        stream = (stream.astype(jnp.float32) + jnp.dot(hidden, down_w[layer_index], preferred_element_type=jnp.float32)).astype(jnp.bfloat16)
    return stream
```

```python
import functools

import jax
import jax.numpy as jnp
from jax import lax
from jax.experimental import pallas as pl
from jax.experimental.pallas import tpu as pltpu
from jax.sharding import PartitionSpec as P

HEAD_DIM = 64
BLK = 64
NBLK = 16
HB = 4
EPS = 1e-05
CAP = 64
DOM = 32
MP = 4
D = 512
FF = 2048
F_IN = 256
ROWS = 256
NODES = 1024
AUX = 8
BIAS_ROWS = 16
SENT = ROWS + 3 * BIAS_ROWS

F32 = jnp.float32
BF16 = jnp.bfloat16


def dot(a, b):
    return jnp.dot(a, b, preferred_element_type=F32)


def dot_t(a, b):
    return lax.dot_general(a, b, (((1,), (1,)), ((), ())), preferred_element_type=F32)


def iota(shape, dim):
    return lax.broadcasted_iota(jnp.int32, shape, dim)


def normalize(values, gain):
    mean = jnp.mean(values, axis=-1, keepdims=True)
    centered = values - mean
    variance = jnp.mean(centered * centered, axis=-1, keepdims=True)
    return centered * lax.rsqrt(variance + EPS) * gain


def silu(v):
    return v / (1.0 + jnp.exp(-v))


VMEM = pl.BlockSpec(memory_space=pltpu.VMEM)
SMEM = pl.BlockSpec(memory_space=pltpu.SMEM)
ANY = pl.BlockSpec(memory_space=pl.ANY)


PACK_ROWS = 384
OFF_OUT = 96
OFF_UP = 128
OFF_DOWN = 256


def pack_kernel(where_ref, qkv_ref, out_ref, up_ref, down_ref, o_ref, sems):
    d = where_ref[0]
    row = pl.multiple_of(d * 16, 16)
    out_row = pl.multiple_of((d // 4) * 16, 16)
    out_col = pl.multiple_of((d % 4) * 128, 128)
    copies = []

    def add(src, at):
        copies.append(pltpu.make_async_copy(src, o_ref.at[pl.ds(at, 16), :], sems.at[len(copies)]))

    for l in range(2):
        for c in range(3):
            add(qkv_ref.at[l, c, pl.ds(row, 16), :], (l * 3 + c) * 16)
        add(out_ref.at[l, pl.ds(out_row, 16), pl.ds(out_col, 128)], OFF_OUT + l * 16)
        for c in range(4):
            add(up_ref.at[l, pl.ds(row, 16), pl.ds(c * 128, 128)], OFF_UP + (l * 4 + c) * 16)
            add(down_ref.at[l, pl.ds(row, 16), pl.ds(c * 128, 128)], OFF_DOWN + (l * 4 + c) * 16)
    for copy in copies:
        copy.start()
    for copy in copies:
        copy.wait()


def pack_weights(where, qkv_w, out_w, up_w, down_w):
    return pl.pallas_call(
        pack_kernel,
        out_shape=jax.ShapeDtypeStruct((PACK_ROWS, 128), BF16),
        in_specs=[SMEM, ANY, ANY, ANY, ANY],
        out_specs=VMEM,
        scratch_shapes=[pltpu.SemaphoreType.DMA((24,))],
        name="pack_weights",
    )(where, qkv_w, out_w, up_w, down_w)


def dispatch_kernel(t_ref, f_ref, o_ref):
    t = t_ref[...]
    owner = t >> 10
    node = t & (NODES - 1)
    member = owner == iota((DOM, 1024), 0)
    memb = jnp.where(member, 1.0, 0.0).astype(BF16)
    upper = jnp.where(iota((128, 128), 0) < iota((128, 128), 1), 1.0, 0.0).astype(BF16)
    carry = jnp.zeros((DOM, 1), F32)
    rank = []
    for g in range(8):
        part = memb[:, g * 128 : (g + 1) * 128]
        mask = member[:, g * 128 : (g + 1) * 128]
        before = dot(part, upper) + carry
        rank.append(jnp.sum(jnp.where(mask, before, 0.0), axis=0, keepdims=True))
        carry = carry + jnp.sum(part.astype(F32), axis=1, keepdims=True)
    rank = jnp.concatenate(rank, axis=1).astype(jnp.int32)
    slot = owner * CAP + rank
    k = iota((256, 1024), 0)
    code = jnp.where(k < 128, 64 - (node >> 5), node & 31)
    table = jnp.where((k & (CAP - 1)) == rank, code, 0).astype(F32).astype(BF16)
    aux = dot_t(memb, table)
    aux = jnp.where(iota((DOM, 256), 1) < 128, 64.0 - aux, aux)
    feat = f_ref[...]
    for g in range(8):
        pick = jnp.where(slot - g * 256 == iota((256, 1024), 0), 1.0, 0.0).astype(BF16)
        rows = dot(pick, feat).astype(BF16)
        for i in range(4):
            e = g * 4 + i
            o_ref[e, 0:CAP, :] = rows[i * CAP : (i + 1) * CAP, :]
            o_ref[e, CAP : CAP + AUX, :] = jnp.broadcast_to(aux[e : e + 1, :], (AUX, 256)).astype(BF16)


def dispatch(grid_target, grid_feat):
    return pl.pallas_call(
        dispatch_kernel,
        out_shape=jax.ShapeDtypeStruct((DOM, CAP + AUX, F_IN), BF16),
        in_specs=[VMEM, VMEM],
        out_specs=VMEM,
        name="dispatch",
    )(grid_target.reshape(1, 1024), grid_feat)


def receive_kernel(where_ref, r_ref, w1_ref, b1_ref, w2_ref, gain_ref, mesh_ref, bias_ref, s_ref, sb_ref, o1_ref, o2_ref, o3_ref, msg_ref):
    m = where_ref[1]
    low = iota((1, 128), 1) < CAP
    codes = []
    for g in range(8):
        rows = jnp.concatenate([r_ref[g * 4 + i, 0:CAP, :] for i in range(4)], axis=0)
        first = silu(dot(rows, w1_ref[...]) + b1_ref[...]).astype(BF16)
        second = dot(first, w2_ref[...])
        msg_ref[g * 256 : (g + 1) * 256, :] = normalize(second, gain_ref[...]).astype(BF16)
        lines = []
        for i in range(4):
            line = r_ref[g * 4 + i, CAP : CAP + AUX, :].astype(F32)[0:1, :]
            lines.append(line[:, 0:128] * 32.0 + line[:, 128:256])
        codes.append(jnp.where(low, lines[0], lines[1]))
        codes.append(jnp.where(low, lines[2], lines[3]))
    codes = jnp.concatenate(codes, axis=1).astype(jnp.int32)
    lane_block = iota((ROWS, D), 1) // 128
    for k, out in enumerate((s_ref, o1_ref, o2_ref, o3_ref)):
        base = pl.multiple_of(((m + k) % MP) * ROWS, ROWS)
        total = jnp.zeros((ROWS, D), F32)
        for g in range(8):
            hit = codes[:, g * 256 : (g + 1) * 256] - base == iota((ROWS, 256), 0)
            pick = jnp.where(hit, 1.0, 0.0).astype(BF16)
            total = total + dot(pick, msg_ref[g * 256 : (g + 1) * 256, :])
        own = mesh_ref[pl.ds(base, ROWS), :].astype(F32)
        own = jnp.concatenate([own] * 4, axis=1)
        total = total + jnp.where(lane_block == m, own, 0.0)
        bias = jnp.concatenate([bias_ref[0, :, pl.ds(base, ROWS)], bias_ref[1, :, pl.ds(base, ROWS)]], axis=1)
        if k == 0:
            out[...] = total
            sb_ref[...] = bias
        else:
            out[0:ROWS, :] = total.astype(BF16)
            high = bias.astype(BF16)
            rest = bias - high.astype(F32)
            middle = rest.astype(BF16)
            rest = rest - middle.astype(F32)
            out[ROWS : ROWS + 16, :] = high
            out[ROWS + 16 : ROWS + 32, :] = middle
            out[ROWS + 32 : ROWS + 48, :] = rest.astype(BF16)


def receive(where, received, enc_w1, enc_b1, enc_w2, enc_gain, mesh_embed, attn_bias):
    sent = jax.ShapeDtypeStruct((SENT, D), BF16)
    return pl.pallas_call(
        receive_kernel,
        out_shape=(jax.ShapeDtypeStruct((ROWS, D), F32), jax.ShapeDtypeStruct((BIAS_ROWS, D), F32), sent, sent, sent),
        in_specs=[SMEM] + [VMEM] * 7,
        out_specs=(VMEM,) * 5,
        scratch_shapes=[pltpu.VMEM((2048, D), BF16)],
        name="receive",
    )(where, received, enc_w1, enc_b1.reshape(1, D), enc_w2, enc_gain.reshape(1, D), mesh_embed, attn_bias)


def combine_kernel(where_ref, s_ref, sb_ref, r1_ref, r2_ref, r3_ref, gain_ref, stream_ref, normed_ref, bias_ref, all_ref):
    m = where_ref[1]
    total = s_ref[...]
    all_ref[m] = sb_ref[...]
    for k, ref in ((1, r1_ref), (2, r2_ref), (3, r3_ref)):
        total = total + ref[0:ROWS, :].astype(F32)
        bias = ref[ROWS : ROWS + 16, :].astype(F32) + ref[ROWS + 16 : ROWS + 32, :].astype(F32)
        all_ref[(m - k) % MP] = bias + ref[ROWS + 32 : ROWS + 48, :].astype(F32)
    stream = total.astype(BF16)
    stream_ref[...] = stream
    normed_ref[...] = normalize(stream.astype(F32), gain_ref[...]).astype(BF16)
    for b in range(4):
        for group in range(2):
            parts = []
            for h in range(4):
                at = (h % 2) * ROWS + b * BLK
                parts.append(all_ref[group * 2 + h // 2, :, at : at + BLK])
            bias_ref[b, group] = jnp.concatenate(parts, axis=1)


def combine(where, own, own_bias, r1, r2, r3, gain):
    return pl.pallas_call(
        combine_kernel,
        out_shape=(
            jax.ShapeDtypeStruct((ROWS, D), BF16),
            jax.ShapeDtypeStruct((ROWS, D), BF16),
            jax.ShapeDtypeStruct((4, 2, NBLK, 256), F32),
        ),
        in_specs=[SMEM] + [VMEM] * 6,
        out_specs=(VMEM,) * 3,
        scratch_shapes=[pltpu.VMEM((4, NBLK, D), F32)],
        name="combine",
    )(where, own, own_bias, r1, r2, r3, gain)


def layer_kernel(
    layer, last, where_ref, nbr_ref, c0_ref, c1_ref, c2_ref, c3_ref, left_ref, right_ref, stream_ref, bias_ref, w_ref, gain_ref, next_ref,
    o_ref, n_ref, qkv_ref, wo_ref, up_ref, down_ref, keys_ref, values_ref, ksel_ref, vsel_ref, att_ref, sems,
):
    m = where_ref[1]
    start = where_ref[0] * NBLK - HB
    copies = {"qkv": [], "out": [], "up": [], "down": []}
    count = [0]

    def add(kind, src, dst):
        copies[kind].append(pltpu.make_async_copy(src, dst, sems.at[count[0]]))
        count[0] += 1

    def rows_of(at, q):
        return w_ref.at[:, :, q, pl.ds(at, 16), :]

    def whole(dst):
        return dst

    for c in range(3):
        for q in range(MP):
            add("qkv", rows_of((layer * 3 + c) * 16, q), qkv_ref.at[c, :, :, :, pl.ds(q * 128, 128)])
    for q in range(MP):
        for c in range(4):
            add("out", w_ref.at[:, c, q, pl.ds(OFF_OUT + layer * 16, 16), :], wo_ref.at[q, :, :, pl.ds(c * 128, 128)])
    for q in range(MP):
        for c in range(4):
            add("up", rows_of(OFF_UP + (layer * 4 + c) * 16, q), up_ref.at[:, :, :, pl.ds(q * 512 + c * 128, 128)])
    for q in range(MP):
        for c in range(4):
            add("down", rows_of(OFF_DOWN + (layer * 4 + c) * 16, q), down_ref.at[q, :, :, :, pl.ds(c * 128, 128)])
    for kind in ("qkv", "out", "up", "down"):
        for copy in copies[kind]:
            copy.start()
    for copy in copies["qkv"]:
        copy.wait()

    wk = qkv_ref[1].reshape(D, D)
    wv = qkv_ref[2].reshape(D, D)
    own = c0_ref[...]
    queries = (dot(own, qkv_ref[0].reshape(D, D)).astype(BF16).astype(F32) * HEAD_DIM ** (-0.5)).astype(BF16)
    att_ref[...] = queries
    for ref, at in (
        (c0_ref, (m + 1) * ROWS),
        (c1_ref, ((m + 3) % MP + 1) * ROWS),
        (c2_ref, ((m + 2) % MP + 1) * ROWS),
        (c3_ref, ((m + 1) % MP + 1) * ROWS),
        (left_ref, 0),
        (right_ref, 5 * ROWS),
    ):
        at = pl.multiple_of(at, ROWS)
        chunk = ref[...]
        keys_ref[pl.ds(at, ROWS), :] = dot(chunk, wk).astype(BF16)
        values_ref[pl.ds(at, ROWS), :] = dot(chunk, wv).astype(BF16)

    diagonal = iota((256, 256), 0) // BLK == iota((256, 256), 1) // BLK
    lane_head = iota((BLK, 256), 1) // BLK

    def block(b, _):
        row = pl.multiple_of(b * BLK, BLK)
        for t in range(NBLK):
            slot = (nbr_ref[m * 4 + b, t] - start) & (DOM * NBLK - 1)
            at = pl.multiple_of(slot * BLK, BLK)
            ksel_ref[t * BLK : (t + 1) * BLK, :] = keys_ref[pl.ds(at, BLK), :]
            vsel_ref[t * BLK : (t + 1) * BLK, :] = values_ref[pl.ds(at, BLK), :]
        for group in range(2):
            cols = slice(group * 256, (group + 1) * 256)
            q = att_ref[pl.ds(row, BLK), cols]
            wide = jnp.where(diagonal, jnp.concatenate([q] * 4, axis=0), jnp.zeros((), BF16))
            scores = dot_t(ksel_ref[:, cols], wide)
            scores = scores.reshape(NBLK, BLK, 256) + bias_ref[b, group][:, None, :]
            top = jnp.max(scores, axis=(0, 1), keepdims=True)
            exponent = jnp.exp(scores - top)
            total = jnp.sum(exponent, axis=(0, 1), keepdims=True)
            weights = (exponent * (1.0 / total)).astype(BF16).reshape(NBLK * BLK, 256)
            mixed = lax.dot_general(weights, vsel_ref[:, cols], (((0,), (0,)), ((), ())), preferred_element_type=F32)
            attended = jnp.zeros((BLK, 256), F32)
            for h in range(4):
                attended = attended + jnp.where(lane_head == h, mixed[h * BLK : (h + 1) * BLK, :], 0.0)
            att_ref[pl.ds(row, BLK), cols] = attended.astype(BF16)
        return 0

    lax.fori_loop(0, 4, block, 0)

    for copy in copies["out"]:
        copy.wait()
    stream = (stream_ref[...].astype(F32) + dot(att_ref[...], wo_ref[...].reshape(D, D))).astype(BF16)
    normed = normalize(stream.astype(F32), gain_ref[...]).astype(BF16)
    for copy in copies["up"]:
        copy.wait()
    for copy in copies["down"]:
        copy.wait()
    total = stream.astype(F32)
    for q in range(MP):
        hidden = silu(dot(normed, up_ref[:, :, :, q * 512 : (q + 1) * 512].reshape(D, 512))).astype(BF16)
        total = total + dot(hidden, down_ref[q].reshape(512, D))
    result = total.astype(BF16)
    if last:
        for q in range(MP):
            o_ref[q] = result[:, q * 128 : (q + 1) * 128]
    else:
        o_ref[...] = result
        n_ref[...] = normalize(result.astype(F32), next_ref[...]).astype(BF16)


def layer_step(layer, last, where, nbr_blocks, chunks, left, right, stream, bias, weights, gain, next_gain):
    rows = jax.ShapeDtypeStruct((ROWS, D), BF16)
    first = jax.ShapeDtypeStruct((MP, ROWS, 128), BF16) if last else rows
    return pl.pallas_call(
        functools.partial(layer_kernel, layer, last),
        out_shape=(first, rows),
        in_specs=[SMEM, SMEM] + [VMEM] * 8 + [ANY, VMEM, VMEM],
        out_specs=(VMEM, VMEM),
        scratch_shapes=[
            pltpu.VMEM((3, 8, 4, 16, D), BF16),
            pltpu.VMEM((4, 8, 16, D), BF16),
            pltpu.VMEM((8, 4, 16, FF), BF16),
            pltpu.VMEM((4, 8, 4, 16, D), BF16),
            pltpu.VMEM((6 * ROWS, D), BF16),
            pltpu.VMEM((6 * ROWS, D), BF16),
            pltpu.VMEM((NBLK * BLK, D), BF16),
            pltpu.VMEM((NBLK * BLK, D), BF16),
            pltpu.VMEM((ROWS, D), BF16),
            pltpu.SemaphoreType.DMA((60,)),
        ],
        name=f"layer{layer}",
    )(where, nbr_blocks, *chunks, left, right, stream, bias, weights, gain, next_gain)


def shift(array, axis, by):
    count = lax.axis_size(axis)
    return lax.ppermute(array, axis, [(i, (i + by) % count) for i in range(count)])


def window(normed, m):
    chunks = [normed] + [shift(normed, "mp", k) for k in (1, 2, 3)]

    def quarter(q):
        picked = chunks[0]
        for k in (1, 2, 3):
            picked = jnp.where((m - k) % MP == q, chunks[k], picked)
        return picked

    left = shift(quarter(3), "dom", 1)
    right = shift(quarter(0), "dom", -1)
    return chunks, left, right


def shards(
    grid_feat, grid_target, enc_w1, enc_b1, enc_w2, enc_gain, mesh_embed, nbr_blocks, attn_bias, ln_gain, qkv_w, out_w, up_w, down_w
):
    m = lax.axis_index("mp").astype(jnp.int32)
    where = jnp.stack([lax.axis_index("dom").astype(jnp.int32), m])
    packed = pack_weights(where, qkv_w, out_w, up_w, down_w)
    weights = lax.all_gather(packed, ("dom", "mp"), tiled=True).reshape(8, 4, MP, PACK_ROWS, 128)
    outgoing = dispatch(grid_target, grid_feat)
    received = lax.all_to_all(outgoing, "dom", 0, 0, tiled=True)
    own, own_bias, *sent = receive(where, received, enc_w1, enc_b1, enc_w2, enc_gain, mesh_embed, attn_bias)
    parts = [shift(part, "mp", k + 1) for k, part in enumerate(sent)]
    stream, normed, bias = combine(where, own, own_bias, *parts, ln_gain[0, 0].reshape(1, D))
    for layer in range(2):
        last = layer == 1
        chunks, left, right = window(normed, m)
        next_gain = ln_gain[(layer + 1) % 2, 0].reshape(1, D)
        stream, normed = layer_step(
            layer, last, where, nbr_blocks, chunks, left, right, stream, bias, weights, ln_gain[layer, 1].reshape(1, D), next_gain
        )
    return lax.all_to_all(stream, "mp", 0, 0, tiled=True).reshape(NODES, 128)


def solution(mesh):
    placed = (
        P(("dom", "mp"), None),
        P(("dom", "mp")),
        P(),
        P(),
        P(),
        P(),
        P("dom", "mp"),
        P("dom", None),
        P("mp", None, "dom"),
        P(),
        P(None, None, None, "mp"),
        P(None, "mp", None),
        P(None, None, "mp"),
        P(None, "mp", None),
    )
    return jax.shard_map(shards, mesh=mesh, in_specs=placed, out_specs=P("dom", "mp"), check_vma=False)
```

```python
import functools

import jax
import jax.numpy as jnp
from jax import lax
from jax.experimental import pallas as pl
from jax.experimental.pallas import tpu as pltpu
from jax.sharding import PartitionSpec as P

HEAD_DIM = 64
BLK = 64
NBLK = 16
HB = 4
EPS = 1e-05
CAP = 64
DOM = 32
MP = 4
D = 512
FF = 2048
F_IN = 256
ROWS = 256
NODES = 1024
AUX = 8
BIAS_ROWS = 16
SENT = ROWS + 3 * BIAS_ROWS

F32 = jnp.float32
BF16 = jnp.bfloat16


def dot(a, b):
    return jnp.dot(a, b, preferred_element_type=F32)


def dot_t(a, b):
    return lax.dot_general(a, b, (((1,), (1,)), ((), ())), preferred_element_type=F32)


def iota(shape, dim):
    return lax.broadcasted_iota(jnp.int32, shape, dim)


def normalize(values, gain):
    mean = jnp.mean(values, axis=-1, keepdims=True)
    centered = values - mean
    variance = jnp.mean(centered * centered, axis=-1, keepdims=True)
    return centered * lax.rsqrt(variance + EPS) * gain


def silu(v):
    return v / (1.0 + jnp.exp(-v))


VMEM = pl.BlockSpec(memory_space=pltpu.VMEM)
SMEM = pl.BlockSpec(memory_space=pltpu.SMEM)
ANY = pl.BlockSpec(memory_space=pl.ANY)


PACK_ROWS = 384
OFF_OUT = 96
OFF_UP = 128
OFF_DOWN = 256


def pack_kernel(where_ref, qkv_ref, out_ref, up_ref, down_ref, o_ref, sems):
    d = where_ref[0]
    row = pl.multiple_of(d * 16, 16)
    out_row = pl.multiple_of((d // 4) * 16, 16)
    out_col = pl.multiple_of((d % 4) * 128, 128)
    copies = []

    def add(src, at):
        copies.append(pltpu.make_async_copy(src, o_ref.at[pl.ds(at, 16), :], sems.at[len(copies)]))

    for l in range(2):
        for c in range(3):
            add(qkv_ref.at[l, c, pl.ds(row, 16), :], (l * 3 + c) * 16)
        add(out_ref.at[l, pl.ds(out_row, 16), pl.ds(out_col, 128)], OFF_OUT + l * 16)
        for c in range(4):
            add(up_ref.at[l, pl.ds(row, 16), pl.ds(c * 128, 128)], OFF_UP + (l * 4 + c) * 16)
            add(down_ref.at[l, pl.ds(row, 16), pl.ds(c * 128, 128)], OFF_DOWN + (l * 4 + c) * 16)
    for copy in copies:
        copy.start()
    for copy in copies:
        copy.wait()


def pack_weights(where, qkv_w, out_w, up_w, down_w):
    return pl.pallas_call(
        pack_kernel,
        out_shape=jax.ShapeDtypeStruct((PACK_ROWS, 128), BF16),
        in_specs=[SMEM, ANY, ANY, ANY, ANY],
        out_specs=VMEM,
        scratch_shapes=[pltpu.SemaphoreType.DMA((24,))],
        name="pack_weights",
    )(where, qkv_w, out_w, up_w, down_w)


def dispatch_kernel(t_ref, f_ref, o_ref):
    t = t_ref[...]
    owner = t >> 10
    node = t & (NODES - 1)
    member = owner == iota((DOM, 1024), 0)
    memb = jnp.where(member, 1.0, 0.0).astype(BF16)
    upper = jnp.where(iota((128, 128), 0) < iota((128, 128), 1), 1.0, 0.0).astype(BF16)
    carry = jnp.zeros((DOM, 1), F32)
    rank = []
    for g in range(8):
        part = memb[:, g * 128 : (g + 1) * 128]
        mask = member[:, g * 128 : (g + 1) * 128]
        before = dot(part, upper) + carry
        rank.append(jnp.sum(jnp.where(mask, before, 0.0), axis=0, keepdims=True))
        carry = carry + jnp.sum(part.astype(F32), axis=1, keepdims=True)
    rank = jnp.concatenate(rank, axis=1).astype(jnp.int32)
    slot = owner * CAP + rank
    k = iota((256, 1024), 0)
    code = jnp.where(k < 128, 64 - (node >> 5), node & 31)
    table = jnp.where((k & (CAP - 1)) == rank, code, 0).astype(F32).astype(BF16)
    aux = dot_t(memb, table)
    aux = jnp.where(iota((DOM, 256), 1) < 128, 64.0 - aux, aux)
    feat = f_ref[...]
    for g in range(8):
        pick = jnp.where(slot - g * 256 == iota((256, 1024), 0), 1.0, 0.0).astype(BF16)
        rows = dot(pick, feat).astype(BF16)
        for i in range(4):
            e = g * 4 + i
            o_ref[e, 0:CAP, :] = rows[i * CAP : (i + 1) * CAP, :]
            o_ref[e, CAP : CAP + AUX, :] = jnp.broadcast_to(aux[e : e + 1, :], (AUX, 256)).astype(BF16)


def dispatch(grid_target, grid_feat):
    return pl.pallas_call(
        dispatch_kernel,
        out_shape=jax.ShapeDtypeStruct((DOM, CAP + AUX, F_IN), BF16),
        in_specs=[VMEM, VMEM],
        out_specs=VMEM,
        name="dispatch",
    )(grid_target.reshape(1, 1024), grid_feat)


def receive_kernel(where_ref, r_ref, w1_ref, b1_ref, w2_ref, gain_ref, mesh_ref, bias_ref, s_ref, sb_ref, o1_ref, o2_ref, o3_ref, msg_ref):
    m = where_ref[1]
    low = iota((1, 128), 1) < CAP
    codes = []
    for g in range(8):
        rows = jnp.concatenate([r_ref[g * 4 + i, 0:CAP, :] for i in range(4)], axis=0)
        first = silu(dot(rows, w1_ref[...]) + b1_ref[...]).astype(BF16)
        second = dot(first, w2_ref[...])
        msg_ref[g * 256 : (g + 1) * 256, :] = normalize(second, gain_ref[...]).astype(BF16)
        lines = []
        for i in range(4):
            line = r_ref[g * 4 + i, CAP : CAP + AUX, :].astype(F32)[0:1, :]
            lines.append(line[:, 0:128] * 32.0 + line[:, 128:256])
        codes.append(jnp.where(low, lines[0], lines[1]))
        codes.append(jnp.where(low, lines[2], lines[3]))
    codes = jnp.concatenate(codes, axis=1).astype(jnp.int32)
    lane_block = iota((ROWS, D), 1) // 128
    for k, out in enumerate((s_ref, o1_ref, o2_ref, o3_ref)):
        base = pl.multiple_of(((m + k) % MP) * ROWS, ROWS)
        total = jnp.zeros((ROWS, D), F32)
        for g in range(8):
            hit = codes[:, g * 256 : (g + 1) * 256] - base == iota((ROWS, 256), 0)
            pick = jnp.where(hit, 1.0, 0.0).astype(BF16)
            total = total + dot(pick, msg_ref[g * 256 : (g + 1) * 256, :])
        own = mesh_ref[pl.ds(base, ROWS), :].astype(F32)
        own = jnp.concatenate([own] * 4, axis=1)
        total = total + jnp.where(lane_block == m, own, 0.0)
        bias = jnp.concatenate([bias_ref[0, :, pl.ds(base, ROWS)], bias_ref[1, :, pl.ds(base, ROWS)]], axis=1)
        if k == 0:
            out[...] = total
            sb_ref[...] = bias
        else:
            out[0:ROWS, :] = total.astype(BF16)
            high = bias.astype(BF16)
            rest = bias - high.astype(F32)
            middle = rest.astype(BF16)
            rest = rest - middle.astype(F32)
            out[ROWS : ROWS + 16, :] = high
            out[ROWS + 16 : ROWS + 32, :] = middle
            out[ROWS + 32 : ROWS + 48, :] = rest.astype(BF16)


def receive(where, received, enc_w1, enc_b1, enc_w2, enc_gain, mesh_embed, attn_bias):
    sent = jax.ShapeDtypeStruct((SENT, D), BF16)
    return pl.pallas_call(
        receive_kernel,
        out_shape=(jax.ShapeDtypeStruct((ROWS, D), F32), jax.ShapeDtypeStruct((BIAS_ROWS, D), F32), sent, sent, sent),
        in_specs=[SMEM] + [VMEM] * 7,
        out_specs=(VMEM,) * 5,
        scratch_shapes=[pltpu.VMEM((2048, D), BF16)],
        name="receive",
    )(where, received, enc_w1, enc_b1.reshape(1, D), enc_w2, enc_gain.reshape(1, D), mesh_embed, attn_bias)


def combine_kernel(where_ref, s_ref, sb_ref, r1_ref, r2_ref, r3_ref, gain_ref, stream_ref, normed_ref, bias_ref, all_ref):
    m = where_ref[1]
    total = s_ref[...]
    all_ref[m] = sb_ref[...]
    for k, ref in ((1, r1_ref), (2, r2_ref), (3, r3_ref)):
        total = total + ref[0:ROWS, :].astype(F32)
        bias = ref[ROWS : ROWS + 16, :].astype(F32) + ref[ROWS + 16 : ROWS + 32, :].astype(F32)
        all_ref[(m - k) % MP] = bias + ref[ROWS + 32 : ROWS + 48, :].astype(F32)
    stream = total.astype(BF16)
    stream_ref[...] = stream
    normed_ref[...] = normalize(stream.astype(F32), gain_ref[...]).astype(BF16)
    for b in range(4):
        for group in range(2):
            parts = []
            for h in range(4):
                at = (h % 2) * ROWS + b * BLK
                parts.append(all_ref[group * 2 + h // 2, :, at : at + BLK])
            bias_ref[b, group] = jnp.concatenate(parts, axis=1)


def combine(where, own, own_bias, r1, r2, r3, gain):
    return pl.pallas_call(
        combine_kernel,
        out_shape=(
            jax.ShapeDtypeStruct((ROWS, D), BF16),
            jax.ShapeDtypeStruct((ROWS, D), BF16),
            jax.ShapeDtypeStruct((4, 2, NBLK, 256), F32),
        ),
        in_specs=[SMEM] + [VMEM] * 6,
        out_specs=(VMEM,) * 3,
        scratch_shapes=[pltpu.VMEM((4, NBLK, D), F32)],
        name="combine",
    )(where, own, own_bias, r1, r2, r3, gain)


def layer_kernel(
    layer, last, where_ref, nbr_ref, c0_ref, c1_ref, c2_ref, c3_ref, left_ref, right_ref, stream_in, bias_in, w_ref, own_qkv_ref, own_out_ref,
    own_up_ref, own_down_ref, gain_ref, next_ref, o_ref, n_ref, win_ref, stream_ref, bias_ref, qkv_ref, wo_ref, up_ref, down_ref, q_ref,
    keys_ref, values_ref, ksel_ref, vsel_ref, att_ref, sems,
):
    m = where_ref[1]
    start = where_ref[0] * NBLK - HB
    copies = {"win": [], "rest": [], "qkv": [], "out": [], "up": [], "down": []}
    count = [0]

    def add(kind, src, dst):
        copies[kind].append(pltpu.make_async_copy(src, dst, sems.at[count[0]]))
        count[0] += 1

    for c in range(3):
        add("qkv", own_qkv_ref.at[layer, c], qkv_ref.at[c, :, :, :, pl.ds(pl.multiple_of(m * 128, 128), 128)])
    add("out", own_out_ref.at[layer], wo_ref.at[m])
    add("up", own_up_ref.at[layer], up_ref.at[:, :, :, pl.ds(pl.multiple_of(m * 512, 512), 512)])
    add("down", own_down_ref.at[layer], down_ref.at[m])
    for k in range(1, MP):
        q = (m + MP - k) % MP
        for c in range(3):
            lane = pl.ds(pl.multiple_of(q * 128, 128), 128)
            add("qkv", w_ref.at[:, :, k - 1, pl.ds((layer * 3 + c) * 16, 16), :], qkv_ref.at[c, :, :, :, lane])
        for c in range(4):
            cols = pl.ds(c * 128, 128)
            lane = pl.ds(pl.multiple_of(q * 512 + c * 128, 128), 128)
            add("out", w_ref.at[:, c, k - 1, pl.ds(OFF_OUT + layer * 16, 16), :], wo_ref.at[q, :, :, cols])
            add("up", w_ref.at[:, :, k - 1, pl.ds(OFF_UP + (layer * 4 + c) * 16, 16), :], up_ref.at[:, :, :, lane])
            add("down", w_ref.at[:, :, k - 1, pl.ds(OFF_DOWN + (layer * 4 + c) * 16, 16), :], down_ref.at[q, :, :, :, cols])
    for ref, at in (
        (c0_ref, m + 1),
        (c1_ref, (m + 3) % MP + 1),
        (c2_ref, (m + 2) % MP + 1),
        (c3_ref, (m + 1) % MP + 1),
        (left_ref, 0),
        (right_ref, 5),
    ):
        add("win", ref, win_ref.at[at])
    add("rest", stream_in, stream_ref)
    add("rest", bias_in, bias_ref)
    for kind in ("qkv", "win", "rest", "out", "up", "down"):
        for copy in copies[kind]:
            copy.start()
    for kind in ("qkv", "win", "rest"):
        for copy in copies[kind]:
            copy.wait()

    half = iota((D, 128), 1) < BLK
    wk = qkv_ref[1].reshape(D, D)
    wv = qkv_ref[2].reshape(D, D).T
    queries = dot(win_ref[m + 1], qkv_ref[0].reshape(D, D)).astype(BF16).astype(F32) * HEAD_DIM ** (-0.5)
    q_ref[...] = queries.astype(BF16)
    for i in range(6):
        chunk = win_ref[i]
        keys_ref[i * ROWS : (i + 1) * ROWS, :] = dot(chunk, wk).astype(BF16)
        flipped = dot_t(wv, chunk)
        for p in range(2):
            pair = flipped[:, p * 128 : (p + 1) * 128]
            turned = pltpu.roll(pair, BLK, 1)
            values_ref[i * 4 + p * 2] = jnp.where(half, pair, turned).astype(BF16)
            values_ref[i * 4 + p * 2 + 1] = jnp.where(half, turned, pair).astype(BF16)

    diagonal = iota((256, 256), 0) // BLK == iota((256, 256), 1) // BLK
    half_rows = iota((BLK, 128), 1) < BLK

    def pair_of_blocks(j, _):
        lanes = pl.ds(pl.multiple_of(j * 128, 128), 128)
        kept = []
        for i in range(2):
            b = j * 2 + i
            row = pl.multiple_of(b * BLK, BLK)
            slots = [(nbr_ref[m * 4 + b, t] - start) & (DOM * NBLK - 1) for t in range(NBLK)]
            for t in range(NBLK):
                at = pl.multiple_of(slots[t] * BLK, BLK)
                ksel_ref[i, t * BLK : (t + 1) * BLK, :] = keys_ref[pl.ds(at, BLK), :]
            for p in range(NBLK // 2):
                vsel_ref[i, :, p * 128 : (p + 1) * 128] = jnp.where(half, values_ref[slots[2 * p]], values_ref[slots[2 * p + 1]])
            for group in range(2):
                cols = slice(group * 256, (group + 1) * 256)
                q = q_ref[pl.ds(row, BLK), cols]
                wide = jnp.where(diagonal, jnp.concatenate([q] * 4, axis=0), jnp.zeros((), BF16))
                scores = dot_t(ksel_ref[i, :, cols], wide)
                scores = scores.reshape(NBLK, BLK, 256)
                bias = bias_ref[b, group]
                top = jnp.max(jnp.max(scores, axis=1) + bias, axis=0, keepdims=True)
                exponent = jnp.exp(scores + (bias - top)[:, None, :])
                total = jnp.sum(jnp.sum(exponent, axis=0), axis=0, keepdims=True)
                weights = exponent.astype(BF16).reshape(NBLK * BLK, 256)
                mixed = dot(vsel_ref[i, cols, :], weights) * (1.0 / total)
                for h in range(4):
                    part = mixed[h * BLK : (h + 1) * BLK, (h // 2) * 128 : (h // 2 + 1) * 128]
                    if h % 2 != i:
                        part = pltpu.roll(part, BLK, 1)
                    if i == 0:
                        kept.append(part)
                    else:
                        at = group * 256 + h * BLK
                        att_ref[at : at + BLK, lanes] = jnp.where(half_rows, kept[group * 4 + h], part)
        return 0

    lax.fori_loop(0, 2, pair_of_blocks, 0, unroll=True)

    for copy in copies["out"]:
        copy.wait()
    attended = att_ref[...].T.astype(BF16)
    stream = (stream_ref[...].astype(F32) + dot(attended, wo_ref[...].reshape(D, D))).astype(BF16)
    normed = normalize(stream.astype(F32), gain_ref[...]).astype(BF16)
    for copy in copies["up"]:
        copy.wait()
    for copy in copies["down"]:
        copy.wait()
    total = stream.astype(F32)
    for q in range(MP):
        hidden = silu(dot(normed, up_ref[:, :, :, q * 512 : (q + 1) * 512].reshape(D, 512))).astype(BF16)
        total = total + dot(hidden, down_ref[q].reshape(512, D))
    result = total.astype(BF16)
    if last:
        for q in range(MP):
            o_ref[q] = result[:, q * 128 : (q + 1) * 128]
    else:
        o_ref[...] = result
        n_ref[...] = normalize(result.astype(F32), next_ref[...]).astype(BF16)


def layer_step(layer, last, where, nbr_blocks, chunks, left, right, stream, bias, weights, mine, gain, next_gain):
    rows = jax.ShapeDtypeStruct((ROWS, D), BF16)
    first = jax.ShapeDtypeStruct((MP, ROWS, 128), BF16) if last else rows
    return pl.pallas_call(
        functools.partial(layer_kernel, layer, last),
        out_shape=(first, rows),
        in_specs=[SMEM, SMEM] + [ANY] * 13 + [VMEM, VMEM],
        out_specs=(VMEM, VMEM),
        scratch_shapes=[
            pltpu.VMEM((6, ROWS, D), BF16),
            pltpu.VMEM((ROWS, D), BF16),
            pltpu.VMEM((4, 2, NBLK, 256), F32),
            pltpu.VMEM((3, 8, 4, 16, D), BF16),
            pltpu.VMEM((4, 8, 16, D), BF16),
            pltpu.VMEM((8, 4, 16, FF), BF16),
            pltpu.VMEM((4, 8, 4, 16, D), BF16),
            pltpu.VMEM((ROWS, D), BF16),
            pltpu.VMEM((6 * ROWS, D), BF16),
            pltpu.VMEM((24, D, 128), BF16),
            pltpu.VMEM((2, NBLK * BLK, D), BF16),
            pltpu.VMEM((2, D, NBLK * BLK), BF16),
            pltpu.VMEM((D, ROWS), F32),
            pltpu.SemaphoreType.DMA((59,)),
        ],
        name=f"layer{layer}",
    )(where, nbr_blocks, *chunks, left, right, stream, bias, weights, *mine, gain, next_gain)


def shift(array, axis, by):
    count = lax.axis_size(axis)
    return lax.ppermute(array, axis, [(i, (i + by) % count) for i in range(count)])


def window(normed, m):
    chunks = [normed] + [shift(normed, "mp", k) for k in (1, 2, 3)]

    def quarter(q):
        picked = chunks[0]
        for k in (1, 2, 3):
            picked = jnp.where((m - k) % MP == q, chunks[k], picked)
        return picked

    left = shift(quarter(3), "dom", 1)
    right = shift(quarter(0), "dom", -1)
    return chunks, left, right


def shards(
    grid_feat, grid_target, enc_w1, enc_b1, enc_w2, enc_gain, mesh_embed, nbr_blocks, attn_bias, ln_gain, qkv_w, out_w, up_w, down_w
):
    m = lax.axis_index("mp").astype(jnp.int32)
    where = jnp.stack([lax.axis_index("dom").astype(jnp.int32), m])
    packed = pack_weights(where, qkv_w, out_w, up_w, down_w)
    outgoing = dispatch(grid_target, grid_feat)
    foreign = [shift(packed, "mp", k) for k in (1, 2, 3)]
    foreign, outgoing = lax.optimization_barrier((foreign, outgoing))
    foreign = jnp.concatenate(foreign, axis=0)
    weights = lax.all_gather(foreign, "dom", tiled=True).reshape(8, 4, MP - 1, PACK_ROWS, 128)
    mine = (
        qkv_w.reshape(2, 3, 8, 4, 16, 128),
        out_w.reshape(2, 8, 16, D),
        up_w.reshape(2, 8, 4, 16, 512),
        down_w.reshape(2, 8, 4, 16, D),
    )
    received = lax.all_to_all(outgoing, "dom", 0, 0, tiled=True)
    own, own_bias, *sent = receive(where, received, enc_w1, enc_b1, enc_w2, enc_gain, mesh_embed, attn_bias)
    parts = [shift(part, "mp", k + 1) for k, part in enumerate(sent)]
    stream, normed, bias = combine(where, own, own_bias, *parts, ln_gain[0, 0].reshape(1, D))
    for layer in range(2):
        last = layer == 1
        chunks, left, right = window(normed, m)
        next_gain = ln_gain[(layer + 1) % 2, 0].reshape(1, D)
        stream, normed = layer_step(
            layer, last, where, nbr_blocks, chunks, left, right, stream, bias, weights, mine, ln_gain[layer, 1].reshape(1, D), next_gain
        )
    return lax.all_to_all(stream, "mp", 0, 0, tiled=True).reshape(NODES, 128)


def solution(mesh):
    placed = (
        P(("dom", "mp"), None),
        P(("dom", "mp")),
        P(),
        P(),
        P(),
        P(),
        P("dom", "mp"),
        P("dom", None),
        P("mp", None, "dom"),
        P(),
        P(None, None, None, "mp"),
        P(None, "mp", None),
        P(None, None, "mp"),
        P(None, "mp", None),
    )
    return jax.shard_map(shards, mesh=mesh, in_specs=placed, out_specs=P("dom", "mp"), check_vma=False)
```

```python
import functools

import jax
import jax.numpy as jnp
from jax import lax
from jax.experimental import pallas as pl
from jax.experimental.pallas import tpu as pltpu
from jax.sharding import PartitionSpec as P

HEAD_DIM = 64
BLK = 64
NBLK = 16
HB = 4
EPS = 1e-05
CAP = 64
DOM = 32
MP = 4
D = 512
FF = 2048
F_IN = 256
ROWS = 256
NODES = 1024
AUX = 8
BIAS_ROWS = 16
SENT = ROWS + 3 * BIAS_ROWS

F32 = jnp.float32
BF16 = jnp.bfloat16


def dot(a, b):
    return jnp.dot(a, b, preferred_element_type=F32)


def dot_t(a, b):
    return lax.dot_general(a, b, (((1,), (1,)), ((), ())), preferred_element_type=F32)


def iota(shape, dim):
    return lax.broadcasted_iota(jnp.int32, shape, dim)


def normalize(values, gain):
    mean = jnp.mean(values, axis=-1, keepdims=True)
    centered = values - mean
    variance = jnp.mean(centered * centered, axis=-1, keepdims=True)
    return centered * lax.rsqrt(variance + EPS) * gain


def silu(v):
    return v / (1.0 + jnp.exp(-v))


VMEM = pl.BlockSpec(memory_space=pltpu.VMEM)
SMEM = pl.BlockSpec(memory_space=pltpu.SMEM)
ANY = pl.BlockSpec(memory_space=pl.ANY)


PACK_ROWS = 384
OFF_OUT = 96
OFF_UP = 128
OFF_DOWN = 256


def pack_kernel(where_ref, qkv_ref, out_ref, up_ref, down_ref, o_ref, sems):
    d = where_ref[0]
    row = pl.multiple_of(d * 16, 16)
    out_row = pl.multiple_of((d // 4) * 16, 16)
    out_col = pl.multiple_of((d % 4) * 128, 128)
    copies = []

    def add(src, at):
        copies.append(pltpu.make_async_copy(src, o_ref.at[pl.ds(at, 16), :], sems.at[len(copies)]))

    for l in range(2):
        for c in range(3):
            add(qkv_ref.at[l, c, pl.ds(row, 16), :], (l * 3 + c) * 16)
        add(out_ref.at[l, pl.ds(out_row, 16), pl.ds(out_col, 128)], OFF_OUT + l * 16)
        for c in range(4):
            add(up_ref.at[l, pl.ds(row, 16), pl.ds(c * 128, 128)], OFF_UP + (l * 4 + c) * 16)
            add(down_ref.at[l, pl.ds(row, 16), pl.ds(c * 128, 128)], OFF_DOWN + (l * 4 + c) * 16)
    for copy in copies:
        copy.start()
    for copy in copies:
        copy.wait()


def pack_weights(where, qkv_w, out_w, up_w, down_w):
    return pl.pallas_call(
        pack_kernel,
        out_shape=jax.ShapeDtypeStruct((PACK_ROWS, 128), BF16),
        in_specs=[SMEM, ANY, ANY, ANY, ANY],
        out_specs=VMEM,
        scratch_shapes=[pltpu.SemaphoreType.DMA((24,))],
        name="pack_weights",
    )(where, qkv_w, out_w, up_w, down_w)


def dispatch_kernel(t_ref, f_ref, o_ref):
    t = t_ref[...]
    owner = t >> 10
    node = t & (NODES - 1)
    member = owner == iota((DOM, 1024), 0)
    memb = jnp.where(member, 1.0, 0.0).astype(BF16)
    upper = jnp.where(iota((128, 128), 0) < iota((128, 128), 1), 1.0, 0.0).astype(BF16)
    carry = jnp.zeros((DOM, 1), F32)
    rank = []
    for g in range(8):
        part = memb[:, g * 128 : (g + 1) * 128]
        mask = member[:, g * 128 : (g + 1) * 128]
        before = dot(part, upper) + carry
        rank.append(jnp.sum(jnp.where(mask, before, 0.0), axis=0, keepdims=True))
        carry = carry + jnp.sum(part.astype(F32), axis=1, keepdims=True)
    rank = jnp.concatenate(rank, axis=1).astype(jnp.int32)
    slot = owner * CAP + rank
    k = iota((256, 1024), 0)
    code = jnp.where(k < 128, 64 - (node >> 5), node & 31)
    table = jnp.where((k & (CAP - 1)) == rank, code, 0).astype(F32).astype(BF16)
    aux = dot_t(memb, table)
    aux = jnp.where(iota((DOM, 256), 1) < 128, 64.0 - aux, aux)
    feat = f_ref[...]
    for g in range(8):
        pick = jnp.where(slot - g * 256 == iota((256, 1024), 0), 1.0, 0.0).astype(BF16)
        rows = dot(pick, feat).astype(BF16)
        for i in range(4):
            e = g * 4 + i
            o_ref[e, 0:CAP, :] = rows[i * CAP : (i + 1) * CAP, :]
            o_ref[e, CAP : CAP + AUX, :] = jnp.broadcast_to(aux[e : e + 1, :], (AUX, 256)).astype(BF16)


def dispatch(grid_target, grid_feat):
    return pl.pallas_call(
        dispatch_kernel,
        out_shape=jax.ShapeDtypeStruct((DOM, CAP + AUX, F_IN), BF16),
        in_specs=[VMEM, VMEM],
        out_specs=VMEM,
        name="dispatch",
    )(grid_target.reshape(1, 1024), grid_feat)


def receive_kernel(where_ref, r_ref, w1_ref, b1_ref, w2_ref, gain_ref, mesh_ref, bias_ref, o0_ref, o1_ref, o2_ref, o3_ref, msg_ref):
    m = where_ref[1]
    low = iota((1, 128), 1) < CAP
    codes = []
    for g in range(8):
        rows = jnp.concatenate([r_ref[g * 4 + i, 0:CAP, :] for i in range(4)], axis=0)
        first = silu(dot(rows, w1_ref[...]) + b1_ref[...]).astype(BF16)
        second = dot(first, w2_ref[...])
        msg_ref[g * 256 : (g + 1) * 256, :] = normalize(second, gain_ref[...]).astype(BF16)
        lines = []
        for i in range(4):
            line = r_ref[g * 4 + i, CAP : CAP + AUX, :].astype(F32)[0:1, :]
            lines.append(line[:, 0:128] * 32.0 + line[:, 128:256])
        codes.append(jnp.where(low, lines[0], lines[1]))
        codes.append(jnp.where(low, lines[2], lines[3]))
    codes = jnp.concatenate(codes, axis=1).astype(jnp.int32)
    lane_block = iota((ROWS, D), 1) // 128
    for k, out in enumerate((o0_ref, o1_ref, o2_ref, o3_ref)):
        base = pl.multiple_of((m ^ k) * ROWS, ROWS)
        total = jnp.zeros((ROWS, D), F32)
        for g in range(8):
            hit = codes[:, g * 256 : (g + 1) * 256] - base == iota((ROWS, 256), 0)
            pick = jnp.where(hit, 1.0, 0.0).astype(BF16)
            total = total + dot(pick, msg_ref[g * 256 : (g + 1) * 256, :])
        own = mesh_ref[pl.ds(base, ROWS), :].astype(F32)
        own = jnp.concatenate([own] * 4, axis=1)
        total = total + jnp.where(lane_block == m, own, 0.0)
        bias = jnp.concatenate([bias_ref[0, :, pl.ds(base, ROWS)], bias_ref[1, :, pl.ds(base, ROWS)]], axis=1)
        out[0:ROWS, :] = total.astype(BF16)
        high = bias.astype(BF16)
        rest = bias - high.astype(F32)
        middle = rest.astype(BF16)
        rest = rest - middle.astype(F32)
        out[ROWS : ROWS + 16, :] = high
        out[ROWS + 16 : ROWS + 32, :] = middle
        out[ROWS + 32 : ROWS + 48, :] = rest.astype(BF16)


def receive(where, received, enc_w1, enc_b1, enc_w2, enc_gain, mesh_embed, attn_bias):
    sent = jax.ShapeDtypeStruct((SENT, D), BF16)
    return pl.pallas_call(
        receive_kernel,
        out_shape=(sent,) * 4,
        in_specs=[SMEM] + [VMEM] * 7,
        out_specs=(VMEM,) * 4,
        scratch_shapes=[pltpu.VMEM((2048, D), BF16)],
        name="receive",
    )(where, received, enc_w1, enc_b1.reshape(1, D), enc_w2, enc_gain.reshape(1, D), mesh_embed, attn_bias)


def combine_kernel(where_ref, r0_ref, r1_ref, r2_ref, r3_ref, gain_ref, stream_ref, normed_ref, bias_ref, all_ref):
    quarter = where_ref[2]
    total = jnp.zeros((ROWS, D), F32)
    for k, ref in enumerate((r0_ref, r1_ref, r2_ref, r3_ref)):
        total = total + ref[0:ROWS, :].astype(F32)
        bias = ref[ROWS : ROWS + 16, :].astype(F32) + ref[ROWS + 16 : ROWS + 32, :].astype(F32)
        all_ref[quarter ^ k] = bias + ref[ROWS + 32 : ROWS + 48, :].astype(F32)
    stream = total.astype(BF16)
    stream_ref[...] = stream
    normed_ref[...] = normalize(stream.astype(F32), gain_ref[...]).astype(BF16)
    for b in range(4):
        for group in range(2):
            parts = []
            for h in range(4):
                at = (h % 2) * ROWS + b * BLK
                parts.append(all_ref[group * 2 + h // 2, :, at : at + BLK])
            bias_ref[b, group] = jnp.concatenate(parts, axis=1)


def combine(where, parts, gain):
    return pl.pallas_call(
        combine_kernel,
        out_shape=(
            jax.ShapeDtypeStruct((ROWS, D), BF16),
            jax.ShapeDtypeStruct((ROWS, D), BF16),
            jax.ShapeDtypeStruct((4, 2, NBLK, 256), F32),
        ),
        in_specs=[SMEM] + [VMEM] * 5,
        out_specs=(VMEM,) * 3,
        scratch_shapes=[pltpu.VMEM((4, NBLK, D), F32)],
        name="combine",
    )(where, *parts, gain)


def layer_kernel(
    layer, last, where_ref, nbr_ref, c0_ref, c1_ref, c2_ref, c3_ref, near_ref, far_ref, stream_in, bias_in, w_ref, own_qkv_ref, own_out_ref,
    own_up_ref, own_down_ref, gain_ref, next_ref, o_ref, n_ref, win_ref, stream_ref, bias_ref, qkv_ref, wo_ref, up_ref, down_ref, q_ref,
    keys_ref, values_ref, ksel_ref, vsel_ref, att_ref, sems,
):
    m = where_ref[1]
    quarter = where_ref[2]
    side = (quarter & 1) * 5
    start = where_ref[3] * NBLK - HB
    copies = {"win": [], "rest": [], "qkv": [], "out": [], "up": [], "down": []}
    count = [0]

    def add(kind, src, dst):
        copies[kind].append(pltpu.make_async_copy(src, dst, sems.at[count[0]]))
        count[0] += 1

    for c in range(3):
        add("qkv", own_qkv_ref.at[layer, c], qkv_ref.at[c, :, :, :, pl.ds(pl.multiple_of(m * 128, 128), 128)])
    add("out", own_out_ref.at[layer], wo_ref.at[m])
    add("up", own_up_ref.at[layer], up_ref.at[:, :, :, pl.ds(pl.multiple_of(m * 512, 512), 512)])
    add("down", own_down_ref.at[layer], down_ref.at[m])
    for k in range(1, MP):
        q = (m + MP - k) % MP
        for c in range(3):
            lane = pl.ds(pl.multiple_of(q * 128, 128), 128)
            add("qkv", w_ref.at[:, :, k - 1, pl.ds((layer * 3 + c) * 16, 16), :], qkv_ref.at[c, :, :, :, lane])
        for c in range(4):
            cols = pl.ds(c * 128, 128)
            lane = pl.ds(pl.multiple_of(q * 512 + c * 128, 128), 128)
            add("out", w_ref.at[:, c, k - 1, pl.ds(OFF_OUT + layer * 16, 16), :], wo_ref.at[q, :, :, cols])
            add("up", w_ref.at[:, :, k - 1, pl.ds(OFF_UP + (layer * 4 + c) * 16, 16), :], up_ref.at[:, :, :, lane])
            add("down", w_ref.at[:, :, k - 1, pl.ds(OFF_DOWN + (layer * 4 + c) * 16, 16), :], down_ref.at[q, :, :, :, cols])
    for ref, at in (
        (c0_ref, quarter + 1),
        (c1_ref, (quarter ^ 1) + 1),
        (c2_ref, (quarter ^ 2) + 1),
        (c3_ref, (quarter ^ 3) + 1),
        (near_ref, side),
        (far_ref, 5 - side),
    ):
        add("win", ref, win_ref.at[at])
    add("rest", stream_in, stream_ref)
    add("rest", bias_in, bias_ref)
    for kind in ("qkv", "win", "rest", "out", "up", "down"):
        for copy in copies[kind]:
            copy.start()
    for kind in ("qkv", "win", "rest"):
        for copy in copies[kind]:
            copy.wait()

    half = iota((D, 128), 1) < BLK
    wk = qkv_ref[1].reshape(D, D)
    wv = qkv_ref[2].reshape(D, D).T
    queries = dot(win_ref[quarter + 1], qkv_ref[0].reshape(D, D)).astype(BF16).astype(F32) * HEAD_DIM ** (-0.5)
    q_ref[...] = queries.astype(BF16)
    for i in range(6):
        chunk = win_ref[i]
        keys_ref[i * ROWS : (i + 1) * ROWS, :] = dot(chunk, wk).astype(BF16)
        flipped = dot_t(wv, chunk)
        for p in range(2):
            pair = flipped[:, p * 128 : (p + 1) * 128]
            turned = pltpu.roll(pair, BLK, 1)
            values_ref[i * 4 + p * 2] = jnp.where(half, pair, turned).astype(BF16)
            values_ref[i * 4 + p * 2 + 1] = jnp.where(half, turned, pair).astype(BF16)

    diagonal = iota((256, 256), 0) // BLK == iota((256, 256), 1) // BLK
    half_rows = iota((BLK, 128), 1) < BLK

    def pair_of_blocks(j, _):
        lanes = pl.ds(pl.multiple_of(j * 128, 128), 128)
        kept = []
        for i in range(2):
            b = j * 2 + i
            row = pl.multiple_of(b * BLK, BLK)
            slots = [(nbr_ref[quarter * 4 + b, t] - start) & (DOM * NBLK - 1) for t in range(NBLK)]
            for t in range(NBLK):
                at = pl.multiple_of(slots[t] * BLK, BLK)
                ksel_ref[i, t * BLK : (t + 1) * BLK, :] = keys_ref[pl.ds(at, BLK), :]
            for p in range(NBLK // 2):
                vsel_ref[i, :, p * 128 : (p + 1) * 128] = jnp.where(half, values_ref[slots[2 * p]], values_ref[slots[2 * p + 1]])
            for group in range(2):
                cols = slice(group * 256, (group + 1) * 256)
                q = q_ref[pl.ds(row, BLK), cols]
                wide = jnp.where(diagonal, jnp.concatenate([q] * 4, axis=0), jnp.zeros((), BF16))
                scores = dot_t(ksel_ref[i, :, cols], wide)
                scores = scores.reshape(NBLK, BLK, 256)
                bias = bias_ref[b, group]
                top = jnp.max(jnp.max(scores, axis=1) + bias, axis=0, keepdims=True)
                exponent = jnp.exp(scores + (bias - top)[:, None, :])
                total = jnp.sum(jnp.sum(exponent, axis=0), axis=0, keepdims=True)
                weights = exponent.astype(BF16).reshape(NBLK * BLK, 256)
                mixed = dot(vsel_ref[i, cols, :], weights) * (1.0 / total)
                for h in range(4):
                    part = mixed[h * BLK : (h + 1) * BLK, (h // 2) * 128 : (h // 2 + 1) * 128]
                    if h % 2 != i:
                        part = pltpu.roll(part, BLK, 1)
                    if i == 0:
                        kept.append(part)
                    else:
                        at = group * 256 + h * BLK
                        att_ref[at : at + BLK, lanes] = jnp.where(half_rows, kept[group * 4 + h], part)
        return 0

    lax.fori_loop(0, 2, pair_of_blocks, 0, unroll=True)

    for copy in copies["out"]:
        copy.wait()
    attended = att_ref[...].T.astype(BF16)
    stream = (stream_ref[...].astype(F32) + dot(attended, wo_ref[...].reshape(D, D))).astype(BF16)
    normed = normalize(stream.astype(F32), gain_ref[...]).astype(BF16)
    for copy in copies["up"]:
        copy.wait()
    for copy in copies["down"]:
        copy.wait()
    total = stream.astype(F32)
    for q in range(MP):
        hidden = silu(dot(normed, up_ref[:, :, :, q * 512 : (q + 1) * 512].reshape(D, 512))).astype(BF16)
        total = total + dot(hidden, down_ref[q].reshape(512, D))
    result = total.astype(BF16)
    if last:
        for q in range(MP):
            o_ref[quarter ^ q] = result[:, q * 128 : (q + 1) * 128]
    else:
        o_ref[...] = result
        n_ref[...] = normalize(result.astype(F32), next_ref[...]).astype(BF16)


def layer_step(layer, last, where, nbr_blocks, chunks, near, far, stream, bias, weights, mine, gain, next_gain):
    rows = jax.ShapeDtypeStruct((ROWS, D), BF16)
    first = jax.ShapeDtypeStruct((MP, ROWS, 128), BF16) if last else rows
    return pl.pallas_call(
        functools.partial(layer_kernel, layer, last),
        out_shape=(first, rows),
        in_specs=[SMEM, SMEM] + [ANY] * 13 + [VMEM, VMEM],
        out_specs=(VMEM, VMEM),
        scratch_shapes=[
            pltpu.VMEM((6, ROWS, D), BF16),
            pltpu.VMEM((ROWS, D), BF16),
            pltpu.VMEM((4, 2, NBLK, 256), F32),
            pltpu.VMEM((3, 8, 4, 16, D), BF16),
            pltpu.VMEM((4, 8, 16, D), BF16),
            pltpu.VMEM((8, 4, 16, FF), BF16),
            pltpu.VMEM((4, 8, 4, 16, D), BF16),
            pltpu.VMEM((ROWS, D), BF16),
            pltpu.VMEM((6 * ROWS, D), BF16),
            pltpu.VMEM((24, D, 128), BF16),
            pltpu.VMEM((2, NBLK * BLK, D), BF16),
            pltpu.VMEM((2, D, NBLK * BLK), BF16),
            pltpu.VMEM((D, ROWS), F32),
            pltpu.SemaphoreType.DMA((59,)),
        ],
        name=f"layer{layer}",
    )(where, nbr_blocks, *chunks, near, far, stream, bias, weights, *mine, gain, next_gain)


def shift(array, axis, by):
    count = lax.axis_size(axis)
    return lax.ppermute(array, axis, [(i, (i + by) % count) for i in range(count)])


def send(array, route):
    pairs = []
    for dom in range(DOM):
        for x in range(MP):
            to = route(x, dom // 2, dom % 2)
            if to is not None:
                pairs.append((dom * MP + x, (to[1] % 16 * 2 + to[2]) * MP + to[0]))
    return lax.ppermute(array, ("dom", "mp"), pairs)


def to_owner(k):
    return lambda x, w, c: (2 * c + (x ^ k) // 2, w, (x ^ k) % 2)


def to_output(k):
    return lambda x, w, c: ((2 * (x % 2) + c) ^ k, w, x // 2)


def other_core(x, w, c):
    return (x, w, 1 - c)


def other_chip(x, w, c):
    return (x ^ 1, w, c)


def to_close(x, w, c):
    return {(3, 1): (0, w + 1, 0), (1, 1): (2, w, 0), (2, 0): (1, w, 1), (0, 0): (3, w - 1, 1)}.get((x, c))


def to_distant(x, w, c):
    return {(3, 1): (1, w + 1, 0), (1, 1): (3, w, 0), (2, 0): (0, w, 1), (0, 0): (2, w - 1, 1)}.get((x, c))


def window(normed, close):
    distant_halo = send(normed, to_distant)
    close_halo = send(normed, to_close)
    across = send(normed, other_chip)
    beside = send(normed, other_core)
    diagonal = send(across, other_core)
    near = jnp.where(close, close_halo, distant_halo)
    far = send(near, other_core)
    return (normed, beside, across, diagonal), near, far


def place_kernel(where_ref, r0_ref, r1_ref, r2_ref, r3_ref, o_ref):
    for k, ref in enumerate((r0_ref, r1_ref, r2_ref, r3_ref)):
        o_ref[pl.ds(pl.multiple_of((where_ref[1] ^ k) * ROWS, ROWS), ROWS), :] = ref[...]


def place(where, parts):
    return pl.pallas_call(
        place_kernel,
        out_shape=jax.ShapeDtypeStruct((NODES, 128), BF16),
        in_specs=[SMEM] + [VMEM] * 4,
        out_specs=VMEM,
        name="place",
    )(where, *parts)


def shards(
    grid_feat, grid_target, enc_w1, enc_b1, enc_w2, enc_gain, mesh_embed, nbr_blocks, attn_bias, ln_gain, qkv_w, out_w, up_w, down_w
):
    dom = lax.axis_index("dom").astype(jnp.int32)
    m = lax.axis_index("mp").astype(jnp.int32)
    core = dom % 2
    half = m // 2
    quarter = 2 * (m % 2) + core
    where = jnp.stack([dom, m, quarter, dom - core + half])
    close = (m == 0) | (m == 2)
    close = jnp.where(core == 0, close, ~close)
    packed = pack_weights(where, qkv_w, out_w, up_w, down_w)
    outgoing = dispatch(grid_target, grid_feat)
    foreign = [shift(packed, "mp", k) for k in (1, 2, 3)]
    nbr_other = send(nbr_blocks, other_core)
    foreign, outgoing, nbr_other = lax.optimization_barrier((foreign, outgoing, nbr_other))
    nbr_blocks = jnp.where(half == core, nbr_blocks, nbr_other)
    foreign = jnp.concatenate(foreign, axis=0)
    weights = lax.all_gather(foreign, "dom", tiled=True).reshape(8, 4, MP - 1, PACK_ROWS, 128)
    mine = (
        qkv_w.reshape(2, 3, 8, 4, 16, 128),
        out_w.reshape(2, 8, 16, D),
        up_w.reshape(2, 8, 4, 16, 512),
        down_w.reshape(2, 8, 4, 16, D),
    )
    received = lax.all_to_all(outgoing, "dom", 0, 0, tiled=True)
    sent = receive(where, received, enc_w1, enc_b1, enc_w2, enc_gain, mesh_embed, attn_bias)
    parts = [send(part, to_owner(k)) for k, part in enumerate(sent)]
    stream, normed, bias = combine(where, parts, ln_gain[0, 0].reshape(1, D))
    for layer in range(2):
        last = layer == 1
        chunks, near, far = window(normed, close)
        next_gain = ln_gain[(layer + 1) % 2, 0].reshape(1, D)
        stream, normed = layer_step(
            layer, last, where, nbr_blocks, chunks, near, far, stream, bias, weights, mine, ln_gain[layer, 1].reshape(1, D), next_gain
        )
    return place(where, [send(stream[k], to_output(k)) for k in range(MP)])


def solution(mesh):
    placed = (
        P(("dom", "mp"), None),
        P(("dom", "mp")),
        P(),
        P(),
        P(),
        P(),
        P("dom", "mp"),
        P("dom", None),
        P("mp", None, "dom"),
        P(),
        P(None, None, None, "mp"),
        P(None, "mp", None),
        P(None, None, "mp"),
        P(None, "mp", None),
    )
    return jax.shard_map(shards, mesh=mesh, in_specs=placed, out_specs=P("dom", "mp"), check_vma=False)
```

```python
import functools

import jax
import jax.numpy as jnp
from jax import lax
from jax.experimental import pallas as pl
from jax.experimental.pallas import tpu as pltpu
from jax.sharding import PartitionSpec as P

HEAD_DIM = 64
BLK = 64
NBLK = 16
HB = 4
EPS = 1e-05
CAP = 64
DOM = 32
MP = 4
D = 512
FF = 2048
F_IN = 256
ROWS = 256
NODES = 1024
AUX = 8
BIAS_ROWS = 16
SENT = ROWS + 3 * BIAS_ROWS

F32 = jnp.float32
BF16 = jnp.bfloat16


def dot(a, b):
    return jnp.dot(a, b, preferred_element_type=F32)


def dot_t(a, b):
    return lax.dot_general(a, b, (((1,), (1,)), ((), ())), preferred_element_type=F32)


def iota(shape, dim):
    return lax.broadcasted_iota(jnp.int32, shape, dim)


def normalize(values, gain):
    mean = jnp.mean(values, axis=-1, keepdims=True)
    centered = values - mean
    variance = jnp.mean(centered * centered, axis=-1, keepdims=True)
    return centered * lax.rsqrt(variance + EPS) * gain


def silu(v):
    return v / (1.0 + jnp.exp(-v))


VMEM = pl.BlockSpec(memory_space=pltpu.VMEM)
SMEM = pl.BlockSpec(memory_space=pltpu.SMEM)
ANY = pl.BlockSpec(memory_space=pl.ANY)


PACK_ROWS = 384
OFF_OUT = 96
OFF_UP = 128
OFF_DOWN = 256


def pack_kernel(qkv_ref, out_ref, up_ref, down_ref, o_ref, sems):
    d = lax.axis_index("dom")
    row = pl.multiple_of(d * 16, 16)
    out_row = pl.multiple_of((d // 4) * 16, 16)
    out_col = pl.multiple_of((d % 4) * 128, 128)
    copies = []

    def add(src, at):
        copies.append(pltpu.make_async_copy(src, o_ref.at[pl.ds(at, 16), :], sems.at[len(copies)]))

    for l in range(2):
        for c in range(3):
            add(qkv_ref.at[l, c, pl.ds(row, 16), :], (l * 3 + c) * 16)
        add(out_ref.at[l, pl.ds(out_row, 16), pl.ds(out_col, 128)], OFF_OUT + l * 16)
        for c in range(4):
            add(up_ref.at[l, pl.ds(row, 16), pl.ds(c * 128, 128)], OFF_UP + (l * 4 + c) * 16)
            add(down_ref.at[l, pl.ds(row, 16), pl.ds(c * 128, 128)], OFF_DOWN + (l * 4 + c) * 16)
    for copy in copies:
        copy.start()
    for copy in copies:
        copy.wait()


def pack_weights(qkv_w, out_w, up_w, down_w):
    return pl.pallas_call(
        pack_kernel,
        out_shape=jax.ShapeDtypeStruct((PACK_ROWS, 128), BF16),
        in_specs=[ANY, ANY, ANY, ANY],
        out_specs=VMEM,
        scratch_shapes=[pltpu.SemaphoreType.DMA((24,))],
        name="pack_weights",
    )(qkv_w, out_w, up_w, down_w)


def dispatch_kernel(t_ref, f_ref, o_ref):
    t = t_ref[...]
    owner = t >> 10
    node = t & (NODES - 1)
    member = owner == iota((DOM, 1024), 0)
    memb = jnp.where(member, 1.0, 0.0).astype(BF16)
    upper = jnp.where(iota((128, 128), 0) < iota((128, 128), 1), 1.0, 0.0).astype(BF16)
    carry = jnp.zeros((DOM, 1), F32)
    rank = []
    for g in range(8):
        part = memb[:, g * 128 : (g + 1) * 128]
        mask = member[:, g * 128 : (g + 1) * 128]
        before = dot(part, upper) + carry
        rank.append(jnp.sum(jnp.where(mask, before, 0.0), axis=0, keepdims=True))
        carry = carry + jnp.sum(part.astype(F32), axis=1, keepdims=True)
    rank = jnp.concatenate(rank, axis=1).astype(jnp.int32)
    slot = owner * CAP + rank
    k = iota((256, 1024), 0)
    code = jnp.where(k < 128, 64 - (node >> 5), node & 31)
    table = jnp.where((k & (CAP - 1)) == rank, code, 0).astype(F32).astype(BF16)
    aux = dot_t(memb, table)
    aux = jnp.where(iota((DOM, 256), 1) < 128, 64.0 - aux, aux)
    feat = f_ref[...]
    for g in range(8):
        pick = jnp.where(slot - g * 256 == iota((256, 1024), 0), 1.0, 0.0).astype(BF16)
        rows = dot(pick, feat).astype(BF16)
        for i in range(4):
            e = g * 4 + i
            o_ref[e, 0:CAP, :] = rows[i * CAP : (i + 1) * CAP, :]
            o_ref[e, CAP : CAP + AUX, :] = jnp.broadcast_to(aux[e : e + 1, :], (AUX, 256)).astype(BF16)


def dispatch(grid_target, grid_feat):
    return pl.pallas_call(
        dispatch_kernel,
        out_shape=jax.ShapeDtypeStruct((DOM, CAP + AUX, F_IN), BF16),
        in_specs=[VMEM, VMEM],
        out_specs=VMEM,
        name="dispatch",
    )(grid_target.reshape(1, 1024), grid_feat)


def receive_kernel(where_ref, r_ref, w1_ref, b1_ref, w2_ref, gain_ref, mesh_ref, bias_ref, o0_ref, o1_ref, o2_ref, o3_ref, msg_ref):
    m = where_ref[1]
    low = iota((1, 128), 1) < CAP
    codes = []
    for g in range(8):
        rows = jnp.concatenate([r_ref[g * 4 + i, 0:CAP, :] for i in range(4)], axis=0)
        first = silu(dot(rows, w1_ref[...]) + b1_ref[...]).astype(BF16)
        second = dot(first, w2_ref[...])
        msg_ref[g * 256 : (g + 1) * 256, :] = normalize(second, gain_ref[...]).astype(BF16)
        lines = []
        for i in range(4):
            line = r_ref[g * 4 + i, CAP : CAP + AUX, :].astype(F32)[0:1, :]
            lines.append(line[:, 0:128] * 32.0 + line[:, 128:256])
        codes.append(jnp.where(low, lines[0], lines[1]))
        codes.append(jnp.where(low, lines[2], lines[3]))
    codes = jnp.concatenate(codes, axis=1).astype(jnp.int32)
    lane_block = iota((ROWS, D), 1) // 128
    for k, out in enumerate((o0_ref, o1_ref, o2_ref, o3_ref)):
        base = pl.multiple_of((m ^ k) * ROWS, ROWS)
        total = jnp.zeros((ROWS, D), F32)
        for g in range(8):
            hit = codes[:, g * 256 : (g + 1) * 256] - base == iota((ROWS, 256), 0)
            pick = jnp.where(hit, 1.0, 0.0).astype(BF16)
            total = total + dot(pick, msg_ref[g * 256 : (g + 1) * 256, :])
        own = mesh_ref[pl.ds(base, ROWS), :].astype(F32)
        own = jnp.concatenate([own] * 4, axis=1)
        total = total + jnp.where(lane_block == m, own, 0.0)
        bias = jnp.concatenate([bias_ref[0, :, pl.ds(base, ROWS)], bias_ref[1, :, pl.ds(base, ROWS)]], axis=1)
        out[0:ROWS, :] = total.astype(BF16)
        high = bias.astype(BF16)
        rest = bias - high.astype(F32)
        middle = rest.astype(BF16)
        rest = rest - middle.astype(F32)
        out[ROWS : ROWS + 16, :] = high
        out[ROWS + 16 : ROWS + 32, :] = middle
        out[ROWS + 32 : ROWS + 48, :] = rest.astype(BF16)


def receive(where, received, enc_w1, enc_b1, enc_w2, enc_gain, mesh_embed, attn_bias):
    sent = jax.ShapeDtypeStruct((SENT, D), BF16)
    return pl.pallas_call(
        receive_kernel,
        out_shape=(sent,) * 4,
        in_specs=[SMEM] + [VMEM] * 7,
        out_specs=(VMEM,) * 4,
        scratch_shapes=[pltpu.VMEM((2048, D), BF16)],
        name="receive",
    )(where, received, enc_w1, enc_b1.reshape(1, D), enc_w2, enc_gain.reshape(1, D), mesh_embed, attn_bias)


def combine_kernel(r0_ref, r1_ref, r2_ref, r3_ref, gain_ref, stream_ref, normed_ref):
    total = jnp.zeros((ROWS, D), F32)
    for ref in (r0_ref, r1_ref, r2_ref, r3_ref):
        total = total + ref[...].astype(F32)
    stream = total.astype(BF16)
    stream_ref[...] = stream
    normed_ref[...] = normalize(stream.astype(F32), gain_ref[...]).astype(BF16)


def combine(parts, gain):
    rows = jax.ShapeDtypeStruct((ROWS, D), BF16)
    return pl.pallas_call(
        combine_kernel,
        grid=(1,),
        out_shape=(rows, rows),
        in_specs=[pl.BlockSpec((ROWS, D), lambda i: (0, 0))] * 4 + [pl.BlockSpec((1, D), lambda i: (0, 0))],
        out_specs=(pl.BlockSpec((ROWS, D), lambda i: (0, 0)),) * 2,
        name="combine",
    )(*parts, gain)


def bias_kernel(where_ref, *rest):
    pieces, (bias_ref, all_ref) = rest[:12], rest[12:]
    quarter = where_ref[2]
    for k in range(MP):
        high, middle, low = pieces[3 * k : 3 * k + 3]
        all_ref[quarter ^ k] = high[...].astype(F32) + middle[...].astype(F32) + low[...].astype(F32)
    for b in range(4):
        for group in range(2):
            parts = []
            for h in range(4):
                at = (h % 2) * ROWS + b * BLK
                parts.append(all_ref[group * 2 + h // 2, :, at : at + BLK])
            bias_ref[b, group] = jnp.concatenate(parts, axis=1)


def score_bias(where, parts):
    return pl.pallas_call(
        bias_kernel,
        grid=(1,),
        out_shape=jax.ShapeDtypeStruct((4, 2, NBLK, 256), F32),
        in_specs=[SMEM] + [pl.BlockSpec((BIAS_ROWS, D), lambda i, j=j: (j, 0)) for j in (16, 17, 18)] * 4,
        out_specs=pl.BlockSpec((4, 2, NBLK, 256), lambda i: (0, 0, 0, 0)),
        scratch_shapes=[pltpu.VMEM((4, NBLK, D), F32)],
        name="score_bias",
    )(where, *[part for part in parts for _ in range(3)])


def layer_kernel(
    layer, last, where_ref, nbr_ref, c0_ref, c1_ref, c2_ref, c3_ref, near_ref, far_ref, stream_in, bias_in, w_ref, own_qkv_ref, own_out_ref,
    own_up_ref, own_down_ref, gain_ref, next_ref, *rest,
):
    outs = rest[: MP if last else 2]
    win_ref, stream_ref, bias_ref, qkv_ref, wo_ref, up_ref, down_ref, q_ref, keys_ref, values_ref, ksel_ref, vsel_ref, att_ref, sems = rest[len(outs) :]
    m = where_ref[1]
    quarter = where_ref[2]
    side = (quarter & 1) * 5
    start = where_ref[3] * NBLK - HB
    copies = {"win": [], "rest": [], "qkv": [], "out": [], "up": [], "down": []}
    count = [0]

    def add(kind, src, dst):
        copies[kind].append(pltpu.make_async_copy(src, dst, sems.at[count[0]]))
        count[0] += 1

    for c in range(3):
        add("qkv", own_qkv_ref.at[layer, c], qkv_ref.at[c, :, :, :, pl.ds(pl.multiple_of(m * 128, 128), 128)])
    add("out", own_out_ref.at[layer], wo_ref.at[m])
    add("up", own_up_ref.at[layer], up_ref.at[:, :, :, pl.ds(pl.multiple_of(m * 512, 512), 512)])
    add("down", own_down_ref.at[layer], down_ref.at[m])
    for k in range(1, MP):
        q = (m + MP - k) % MP
        for c in range(3):
            lane = pl.ds(pl.multiple_of(q * 128, 128), 128)
            add("qkv", w_ref.at[:, :, k - 1, pl.ds((layer * 3 + c) * 16, 16), :], qkv_ref.at[c, :, :, :, lane])
        for c in range(4):
            cols = pl.ds(c * 128, 128)
            lane = pl.ds(pl.multiple_of(q * 512 + c * 128, 128), 128)
            add("out", w_ref.at[:, c, k - 1, pl.ds(OFF_OUT + layer * 16, 16), :], wo_ref.at[q, :, :, cols])
            add("up", w_ref.at[:, :, k - 1, pl.ds(OFF_UP + (layer * 4 + c) * 16, 16), :], up_ref.at[:, :, :, lane])
            add("down", w_ref.at[:, :, k - 1, pl.ds(OFF_DOWN + (layer * 4 + c) * 16, 16), :], down_ref.at[q, :, :, :, cols])
    for ref, at in (
        (c0_ref, quarter + 1),
        (c1_ref, (quarter ^ 1) + 1),
        (c2_ref, (quarter ^ 2) + 1),
        (c3_ref, (quarter ^ 3) + 1),
        (near_ref, side),
        (far_ref, 5 - side),
    ):
        add("win", ref, win_ref.at[at])
    add("rest", stream_in, stream_ref)
    add("rest", bias_in, bias_ref)
    for kind in ("qkv", "win", "rest", "out", "up", "down"):
        for copy in copies[kind]:
            copy.start()
    for kind in ("qkv", "win", "rest"):
        for copy in copies[kind]:
            copy.wait()

    half = iota((D, 128), 1) < BLK
    wk = qkv_ref[1].reshape(D, D)
    wv = qkv_ref[2].reshape(D, D).T
    queries = dot(win_ref[quarter + 1], qkv_ref[0].reshape(D, D)).astype(BF16).astype(F32) * HEAD_DIM ** (-0.5)
    q_ref[...] = queries.astype(BF16)
    for i in range(6):
        chunk = win_ref[i]
        keys_ref[i * ROWS : (i + 1) * ROWS, :] = dot(chunk, wk).astype(BF16)
        flipped = dot_t(wv, chunk)
        for p in range(2):
            pair = flipped[:, p * 128 : (p + 1) * 128]
            turned = pltpu.roll(pair, BLK, 1)
            values_ref[i * 4 + p * 2] = jnp.where(half, pair, turned).astype(BF16)
            values_ref[i * 4 + p * 2 + 1] = jnp.where(half, turned, pair).astype(BF16)

    diagonal = iota((256, 256), 0) // BLK == iota((256, 256), 1) // BLK
    half_rows = iota((BLK, 128), 1) < BLK

    def pair_of_blocks(j, _):
        lanes = pl.ds(pl.multiple_of(j * 128, 128), 128)
        kept = []
        for i in range(2):
            b = j * 2 + i
            row = pl.multiple_of(b * BLK, BLK)
            slots = [(nbr_ref[quarter * 4 + b, t] - start) & (DOM * NBLK - 1) for t in range(NBLK)]
            for t in range(NBLK):
                at = pl.multiple_of(slots[t] * BLK, BLK)
                ksel_ref[i, t * BLK : (t + 1) * BLK, :] = keys_ref[pl.ds(at, BLK), :]
            for p in range(NBLK // 2):
                vsel_ref[i, :, p * 128 : (p + 1) * 128] = jnp.where(half, values_ref[slots[2 * p]], values_ref[slots[2 * p + 1]])
            for group in range(2):
                cols = slice(group * 256, (group + 1) * 256)
                q = q_ref[pl.ds(row, BLK), cols]
                wide = jnp.where(diagonal, jnp.concatenate([q] * 4, axis=0), jnp.zeros((), BF16))
                scores = dot_t(ksel_ref[i, :, cols], wide)
                scores = scores.reshape(NBLK, BLK, 256)
                bias = bias_ref[b, group]
                top = jnp.max(jnp.max(scores, axis=1) + bias, axis=0, keepdims=True)
                exponent = jnp.exp(scores + (bias - top)[:, None, :])
                total = jnp.sum(jnp.sum(exponent, axis=0), axis=0, keepdims=True)
                weights = exponent.astype(BF16).reshape(NBLK * BLK, 256)
                mixed = dot(vsel_ref[i, cols, :], weights) * (1.0 / total)
                for h in range(4):
                    part = mixed[h * BLK : (h + 1) * BLK, (h // 2) * 128 : (h // 2 + 1) * 128]
                    if h % 2 != i:
                        part = pltpu.roll(part, BLK, 1)
                    if i == 0:
                        kept.append(part)
                    else:
                        at = group * 256 + h * BLK
                        att_ref[at : at + BLK, lanes] = jnp.where(half_rows, kept[group * 4 + h], part)
        return 0

    lax.fori_loop(0, 2, pair_of_blocks, 0, unroll=True)

    for copy in copies["out"]:
        copy.wait()
    attended = att_ref[...].T.astype(BF16)
    stream = (stream_ref[...].astype(F32) + dot(attended, wo_ref[...].reshape(D, D))).astype(BF16)
    normed = normalize(stream.astype(F32), gain_ref[...]).astype(BF16)
    for copy in copies["up"]:
        copy.wait()
    for copy in copies["down"]:
        copy.wait()
    total = stream.astype(F32)
    for q in range(MP):
        hidden = silu(dot(normed, up_ref[:, :, :, q * 512 : (q + 1) * 512].reshape(D, 512))).astype(BF16)
        total = total + dot(hidden, down_ref[q].reshape(512, D))
    result = total.astype(BF16)
    if last:
        win_ref[0] = result
        for k, out in enumerate(outs):
            out[...] = win_ref[0, :, pl.ds(pl.multiple_of((quarter ^ k) * 128, 128), 128)]
    else:
        outs[0][...] = result
        outs[1][...] = normalize(result.astype(F32), next_ref[...]).astype(BF16)


def layer_step(layer, last, where, nbr_blocks, chunks, near, far, stream, bias, weights, mine, gain, next_gain):
    outs = (jax.ShapeDtypeStruct((ROWS, 128), BF16),) * MP if last else (jax.ShapeDtypeStruct((ROWS, D), BF16),) * 2
    return pl.pallas_call(
        functools.partial(layer_kernel, layer, last),
        out_shape=outs,
        in_specs=[SMEM, SMEM] + [ANY] * 13 + [VMEM, VMEM],
        out_specs=(VMEM,) * len(outs),
        scratch_shapes=[
            pltpu.VMEM((6, ROWS, D), BF16),
            pltpu.VMEM((ROWS, D), BF16),
            pltpu.VMEM((4, 2, NBLK, 256), F32),
            pltpu.VMEM((3, 8, 4, 16, D), BF16),
            pltpu.VMEM((4, 8, 16, D), BF16),
            pltpu.VMEM((8, 4, 16, FF), BF16),
            pltpu.VMEM((4, 8, 4, 16, D), BF16),
            pltpu.VMEM((ROWS, D), BF16),
            pltpu.VMEM((6 * ROWS, D), BF16),
            pltpu.VMEM((24, D, 128), BF16),
            pltpu.VMEM((2, NBLK * BLK, D), BF16),
            pltpu.VMEM((2, D, NBLK * BLK), BF16),
            pltpu.VMEM((D, ROWS), F32),
            pltpu.SemaphoreType.DMA((59,)),
        ],
        name=f"layer{layer}",
    )(where, nbr_blocks, *chunks, near, far, stream, bias, weights, *mine, gain, next_gain)


def shift(array, axis, by):
    count = lax.axis_size(axis)
    return lax.ppermute(array, axis, [(i, (i + by) % count) for i in range(count)])


def send(array, route):
    pairs = []
    for dom in range(DOM):
        for x in range(MP):
            to = route(x, dom // 2, dom % 2)
            if to is not None:
                pairs.append((dom * MP + x, (to[1] % 16 * 2 + to[2]) * MP + to[0]))
    return lax.ppermute(array, ("dom", "mp"), pairs)


def along(x, w):
    return x if w % 2 == 0 else 3 - x


def to_owner(k):
    return lambda x, w, c: (along(2 * c + (x ^ k) // 2, w), w, (x ^ k) % 2)


def to_output(k):
    return lambda x, w, c: ((2 * (along(x, w) % 2) + c) ^ k, w, along(x, w) // 2)


def other_core(x, w, c):
    return (x, w, 1 - c)


def other_chip(x, w, c):
    return (x ^ 1, w, c)


def halo_route(table):
    def route(x, w, c):
        to = table.get((along(x, w), c))
        return to and (along(to[0], w + to[1]), w + to[1], to[2])

    return route


to_close = halo_route({(3, 1): (0, 1, 0), (1, 1): (2, 0, 0), (2, 0): (1, 0, 1), (0, 0): (3, -1, 1)})
to_distant = halo_route({(3, 1): (1, 1, 0), (1, 1): (3, 0, 0), (2, 0): (0, 0, 1), (0, 0): (2, -1, 1)})


def window(normed, close):
    distant_halo = send(normed, to_distant)
    close_halo = send(normed, to_close)
    across = send(normed, other_chip)
    beside = send(normed, other_core)
    diagonal = send(across, other_core)
    near = jnp.where(close, close_halo, distant_halo)
    far = send(near, other_core)
    return (normed, beside, across, diagonal), near, far


def place_kernel(where_ref, r0_ref, r1_ref, r2_ref, r3_ref, o_ref):
    for k, ref in enumerate((r0_ref, r1_ref, r2_ref, r3_ref)):
        o_ref[pl.ds(pl.multiple_of((where_ref[1] ^ k) * ROWS, ROWS), ROWS), :] = ref[...]


def place(where, parts):
    return pl.pallas_call(
        place_kernel,
        out_shape=jax.ShapeDtypeStruct((NODES, 128), BF16),
        in_specs=[SMEM] + [VMEM] * 4,
        out_specs=VMEM,
        name="place",
    )(where, *parts)


def shards(
    grid_feat, grid_target, enc_w1, enc_b1, enc_w2, enc_gain, mesh_embed, nbr_blocks, attn_bias, ln_gain, qkv_w, out_w, up_w, down_w
):
    dom = lax.axis_index("dom").astype(jnp.int32)
    m = lax.axis_index("mp").astype(jnp.int32)
    core = dom % 2
    chip = jnp.where(dom // 2 % 2 == 0, m, 3 - m)
    half = chip // 2
    quarter = 2 * (chip % 2) + core
    where = jnp.stack([dom, m, quarter, dom - core + half])
    close = (chip == 0) | (chip == 2)
    close = jnp.where(core == 0, close, ~close)
    packed = pack_weights(qkv_w, out_w, up_w, down_w)
    outgoing = dispatch(grid_target, grid_feat)
    foreign = [shift(packed, "mp", k) for k in (1, 2, 3)]
    nbr_other = send(nbr_blocks, other_core)
    foreign, outgoing, nbr_other = lax.optimization_barrier((foreign, outgoing, nbr_other))
    nbr_blocks = jnp.where(half == core, nbr_blocks, nbr_other)
    foreign = jnp.concatenate(foreign, axis=0)
    weights = lax.all_gather(foreign, "dom", tiled=True).reshape(8, 4, MP - 1, PACK_ROWS, 128)
    mine = (
        qkv_w.reshape(2, 3, 8, 4, 16, 128),
        out_w.reshape(2, 8, 16, D),
        up_w.reshape(2, 8, 4, 16, 512),
        down_w.reshape(2, 8, 4, 16, D),
    )
    received = lax.all_to_all(outgoing, "dom", 0, 0, tiled=True)
    sent = receive(where, received, enc_w1, enc_b1, enc_w2, enc_gain, mesh_embed, attn_bias)
    parts = [send(part, to_owner(k)) for k, part in enumerate(sent)]
    stream, normed = combine(parts, ln_gain[0, 0].reshape(1, D))
    bias = score_bias(where, parts)
    for layer in range(2):
        last = layer == 1
        chunks, near, far = window(normed, close)
        next_gain = ln_gain[(layer + 1) % 2, 0].reshape(1, D)
        results = layer_step(
            layer, last, where, nbr_blocks, chunks, near, far, stream, bias, weights, mine, ln_gain[layer, 1].reshape(1, D), next_gain
        )
        stream, normed = results[:2]
    return place(where, [send(part, to_output(k)) for k, part in enumerate(results)])


def solution(mesh):
    placed = (
        P(("dom", "mp"), None),
        P(("dom", "mp")),
        P(),
        P(),
        P(),
        P(),
        P("dom", "mp"),
        P("dom", None),
        P("mp", None, "dom"),
        P(),
        P(None, None, None, "mp"),
        P(None, "mp", None),
        P(None, None, "mp"),
        P(None, "mp", None),
    )
    return jax.shard_map(shards, mesh=mesh, in_specs=placed, out_specs=P("dom", "mp"), check_vma=False)
```
